64 devices in a mesh: rep: 4 (over x, y), dp: 16 (over z, core).
Axes of the slice: x: 2, y: 2, z: 8, core: 2. Of those that a mesh axis runs over, the one named last changes fastest.
The devices are a block of a 4x4x8 slice.
Arguments:
- x: bfloat16 [64, 2048, 512], P(('rep', 'dp')), parts along dimension 0
- dy: bfloat16 [64, 2048, 512], P(('rep', 'dp')), parts along dimension 0
- wq: bfloat16 [2, 512, 512], P(None, 'dp')
- wk: bfloat16 [2, 512, 128], P(None, 'dp')
- wv: bfloat16 [2, 512, 128], P(None, 'dp')
- wo: bfloat16 [2, 512, 512], P(None, 'dp')
- w_gate: bfloat16 [2, 512, 1536], P(None, 'dp')
- w_up: bfloat16 [2, 512, 1536], P(None, 'dp')
- w_down: bfloat16 [2, 1536, 512], P(None, 'dp')
- m_wq: float32 [2, 512, 512], P(None, 'dp')
- m_wk: float32 [2, 512, 128], P(None, 'dp')
- m_wv: float32 [2, 512, 128], P(None, 'dp')
- m_wo: float32 [2, 512, 512], P(None, 'dp')
- m_w_gate: float32 [2, 512, 1536], P(None, 'dp')
- m_w_up: float32 [2, 512, 1536], P(None, 'dp')
- m_w_down: float32 [2, 1536, 512], P(None, 'dp')
- v_wq: float32 [2, 512, 512], P(None, 'dp')
- v_wk: float32 [2, 512, 128], P(None, 'dp')
- v_wv: float32 [2, 512, 128], P(None, 'dp')
- v_wo: float32 [2, 512, 512], P(None, 'dp')
- v_w_gate: float32 [2, 512, 1536], P(None, 'dp')
- v_w_up: float32 [2, 512, 1536], P(None, 'dp')
- v_w_down: float32 [2, 1536, 512], P(None, 'dp')
Outputs:
- output 1: bfloat16 [8, 512, 512], P('rep', 'dp'), parts along dimension 0
- output 2: bfloat16 [8, 512, 128], P('rep', 'dp'), parts along dimension 0
- output 3: bfloat16 [8, 512, 128], P('rep', 'dp'), parts along dimension 0
- output 4: bfloat16 [8, 512, 512], P('rep', 'dp'), parts along dimension 0
- output 5: bfloat16 [8, 512, 1536], P('rep', 'dp'), parts along dimension 0
- output 6: bfloat16 [8, 512, 1536], P('rep', 'dp'), parts along dimension 0
- output 7: bfloat16 [8, 1536, 512], P('rep', 'dp'), parts along dimension 0
- output 8: float32 [8, 512, 512], P('rep', 'dp'), parts along dimension 0
- output 9: float32 [8, 512, 128], P('rep', 'dp'), parts along dimension 0
- output 10: float32 [8, 512, 128], P('rep', 'dp'), parts along dimension 0
- output 11: float32 [8, 512, 512], P('rep', 'dp'), parts along dimension 0
- output 12: float32 [8, 512, 1536], P('rep', 'dp'), parts along dimension 0
- output 13: float32 [8, 512, 1536], P('rep', 'dp'), parts along dimension 0
- output 14: float32 [8, 1536, 512], P('rep', 'dp'), parts along dimension 0
- output 15: float32 [8, 512, 512], P('rep', 'dp'), parts along dimension 0
- output 16: float32 [8, 512, 128], P('rep', 'dp'), parts along dimension 0
- output 17: float32 [8, 512, 128], P('rep', 'dp'), parts along dimension 0
- output 18: float32 [8, 512, 512], P('rep', 'dp'), parts along dimension 0
- output 19: float32 [8, 512, 1536], P('rep', 'dp'), parts along dimension 0
- output 20: float32 [8, 512, 1536], P('rep', 'dp'), parts along dimension 0
- output 21: float32 [8, 1536, 512], P('rep', 'dp'), parts along dimension 0
There are 4 independent parts. The reference program is written for one: setup_inputs(seed, part) draws one part's arguments, and reference() takes and returns one part's arrays. A program takes and returns all parts, laid end to end along the dimension named above; an argument that names none is the same for every part.
All inputs are finite; a program needn't handle non-finite values.
Results may differ from the reference program's by a relative error of at most 0.0243.
Values are sent between devices in bfloat16 or wider.
A program may use at most 768 MiB of HBM per device.

```python
import jax
import jax.numpy as jnp
from jax import lax

SEQUENCES = 16
TOKENS = 2048
D = 512
HEADS = 4
KV_HEADS = 1
HEAD = 128
FF = 1536
LAYERS = 2
THETA = 10000
NAMES = ("wq", "wk", "wv", "wo", "w_gate", "w_up", "w_down")
SHAPES = {
    "wq": (LAYERS, D, HEADS * HEAD),
    "wk": (LAYERS, D, KV_HEADS * HEAD),
    "wv": (LAYERS, D, KV_HEADS * HEAD),
    "wo": (LAYERS, HEADS * HEAD, D),
    "w_gate": (LAYERS, D, FF),
    "w_up": (LAYERS, D, FF),
    "w_down": (LAYERS, FF, D),
}


def bump(key, n, height):
    away = (jnp.arange(n, dtype=jnp.int32) - jax.random.randint(key, (), 0, n, jnp.int32)) % n
    return jnp.where(away < n // 8, height, 1.0)


def together(key, own, strength):
    shared = jax.random.normal(key, own.shape[1:], jnp.float32)
    return (own + strength * shared) * lax.rsqrt(1 + strength * strength)


def setup_inputs(seed: int = 0, part: int = 0) -> dict:
    kx, kdy, ka, kb, kz, kf, kh, kl, *keys = jax.random.split(jax.random.key(seed), 8 + 3 * len(NAMES))
    kx, kdy, ka, kb = (jax.random.fold_in(k, part) for k in (kx, kdy, ka, kb))
    kw, km, kv = (keys[i::3] for i in range(3))
    shape = (SEQUENCES, TOKENS, D)
    much_x, much_dy = jax.random.uniform(kz, (2,), jnp.float32, 0.0, 1.0)
    loud = 2.0 ** jax.random.uniform(jax.random.fold_in(kz, 1), (), jnp.float32, -1.0, 2.0)
    layers = 2.0 ** jax.random.uniform(kl, (LAYERS, 1, 1), jnp.float32, -1.0, 1.0)
    times = {"wq": 1.0, "wk": 1.0, "wv": 2.0, "wo": layers, "w_gate": 1.0, "w_up": bump(kh, FF, 4.0), "w_down": layers}
    x = together(ka, jax.random.normal(kx, shape, jnp.float32), much_x) * bump(kf, D, 4.0)
    dy = together(kb, jax.random.normal(kdy, shape, jnp.float32), much_dy)
    drawn = {"x": x.astype(jnp.bfloat16), "dy": (loud * dy * (SEQUENCES * TOKENS) ** -0.5).astype(jnp.bfloat16)}
    for key, name in zip(kw, NAMES, strict=True):
        drawn[name] = (jax.random.normal(key, SHAPES[name], jnp.float32) * SHAPES[name][1] ** -0.5 * times[name]).astype(jnp.bfloat16)
    for key, name in zip(km, NAMES, strict=True):
        drawn[f"m_{name}"] = 0.1 * jax.random.normal(key, SHAPES[name], jnp.float32)
    for key, name in zip(kv, NAMES, strict=True):
        drawn[f"v_{name}"] = jax.random.uniform(key, SHAPES[name], jnp.float32, 0.02, 0.06)
    return drawn


def matmul(a, w):
    return jnp.dot(a, w, preferred_element_type=jnp.float32).astype(jnp.bfloat16)


def normed(h):
    wide = h.astype(jnp.float32)
    scale = lax.rsqrt(jnp.mean(wide**2, -1, keepdims=True) + 1e-6)
    return (wide * scale).astype(jnp.bfloat16)


def turned(t, theta):
    half = t.shape[-1] // 2
    angle = jnp.arange(t.shape[0], dtype=jnp.float32)[:, None] * theta ** (-jnp.arange(half, dtype=jnp.float32) / half)
    cos, sin = jnp.cos(angle)[:, None], jnp.sin(angle)[:, None]
    a, b = t[..., :half].astype(jnp.float32), t[..., half:].astype(jnp.float32)
    return jnp.concatenate([a * cos - b * sin, b * cos + a * sin], -1).astype(jnp.bfloat16)


def seen_by(q, k, v):
    tokens, kv = q.shape[0], k.shape[1]
    q = q.reshape(tokens, kv, -1, q.shape[-1])
    scores = jnp.einsum("tgsd,ugd->gstu", q.astype(jnp.float32), k.astype(jnp.float32)) * q.shape[-1] ** -0.5
    place = jnp.arange(tokens)
    weights = jax.nn.softmax(jnp.where(place[:, None] >= place, scores, -jnp.inf), -1).astype(jnp.bfloat16)
    return jnp.einsum("gstu,ugd->tgsd", weights.astype(jnp.float32), v.astype(jnp.float32)).astype(jnp.bfloat16).reshape(tokens, -1)


def layer(h, w):
    a = normed(h)
    q, k = (turned(matmul(a, w[name]).reshape(h.shape[0], -1, HEAD), THETA) for name in ("wq", "wk"))
    h = h + matmul(seen_by(q, k, matmul(a, w["wv"]).reshape(h.shape[0], -1, HEAD)), w["wo"])
    b = normed(h)
    gate = jnp.dot(b, w["w_gate"], preferred_element_type=jnp.float32)
    up = jnp.dot(b, w["w_up"], preferred_element_type=jnp.float32)
    return h + matmul((jax.nn.silu(gate) * up).astype(jnp.bfloat16), w["w_down"])


def adamw(w, m, v, g):
    m = 0.9 * m + 0.1 * g
    v = 0.95 * v + 0.05 * g * g
    step = m * lax.rsqrt(v + 1e-8) + 0.1 * w
    return (w - 0.02 * step).astype(jnp.bfloat16), m, v


def clipped(gradients, sum_of_squares, count):
    factor = jnp.minimum(1.0, 0.5 * lax.rsqrt(sum_of_squares / count + 1e-30))
    return [g * factor for g in gradients]


def stack(weights, h):
    return lax.scan(lambda h, w: (layer(h, w), None), h, weights)[0]


def reference(x, dy, wq, wk, wv, wo, w_gate, w_up, w_down, m_wq, m_wk, m_wv, m_wo, m_w_gate, m_w_up, m_w_down, v_wq, v_wk, v_wv, v_wo, v_w_gate, v_w_up, v_w_down):
    weights = dict(zip(NAMES, (wq, wk, wv, wo, w_gate, w_up, w_down), strict=True))

    def take(so_far, sequence):
        h, by_y = sequence
        _, back = jax.vjp(stack, weights, h)
        by_weights, by_h = back(by_y)
        return jax.tree.map(lambda total, term: total + term.astype(jnp.float32), so_far, by_weights), by_h

    none_yet = {name: jnp.zeros(w.shape, jnp.float32) for name, w in weights.items()}
    by_weights, by_x = lax.scan(take, none_yet, (x, dy))
    gradients = [by_weights[name].astype(jnp.bfloat16).astype(jnp.float32) for name in NAMES]
    gradients = clipped(gradients, sum(jnp.sum(g * g) for g in gradients), sum(g.size for g in gradients))
    first = (m_wq, m_wk, m_wv, m_wo, m_w_gate, m_w_up, m_w_down)
    second = (v_wq, v_wk, v_wv, v_wo, v_w_gate, v_w_up, v_w_down)
    new = [adamw(weights[name].astype(jnp.float32), m, v, g) for name, m, v, g in zip(NAMES, first, second, gradients, strict=True)]
    return tuple(one[which] for which in range(3) for one in new)
```

```python
import functools

import jax
import jax.numpy as jnp
from jax import lax
from jax.experimental import pallas as pl
from jax.experimental.pallas import tpu as pltpu
from jax.sharding import PartitionSpec as P

HEAD = 128
THETA = 10000
NEG = -1e30
HIDDEN = 2 * NEG
LOG2E = 1.4426950408889634
VMEM = 60 * 2**20
NAMES = ("wq", "wk", "wv", "wo", "w_gate", "w_up", "w_down")
F32, BF16 = jnp.float32, jnp.bfloat16


def _dot(a, b, ca, cb):
    return lax.dot_general(a, b, (((ca,), (cb,)), ((), ())), preferred_element_type=F32)


def _scale(wide):
    return lax.rsqrt(jnp.mean(wide * wide, -1, keepdims=True) + 1e-6)


def _normed(wide):
    return (wide * _scale(wide)).astype(BF16)


def _norm_back(wide, by, by_out):
    by = by.astype(BF16).astype(F32)
    s = _scale(wide)
    inner = s * by - wide * (s * s * s * jnp.mean(wide * by, -1, keepdims=True))
    return (by_out + inner.astype(BF16).astype(F32)).astype(BF16)


def _call(body, grid, ins, outs, shapes, scratch=(), flops=0, size=0, exps=0, comm=None):
    return pl.pallas_call(
        body,
        grid=grid,
        in_specs=ins,
        out_specs=outs,
        out_shape=shapes,
        scratch_shapes=list(scratch),
        compiler_params=pltpu.CompilerParams(dimension_semantics=("arbitrary",) * len(grid), vmem_limit_bytes=VMEM, collective_id=comm,
                                             has_side_effects=comm is not None),
        cost_estimate=pl.CostEstimate(flops=flops, bytes_accessed=size, transcendentals=exps),
    )


def _whole(*shape):
    return pl.BlockSpec(shape, lambda i: (0,) * len(shape), pipeline_mode=pl.Buffered(1))


def _rows(n, *rest):
    return pl.BlockSpec((n, *rest), lambda i: (i,) + (0,) * len(rest))


def _heads(h, n, *rest):
    return pl.BlockSpec((h, n, *rest), lambda i: (0, i) + (0,) * len(rest))


def _out(*shape):
    return jax.ShapeDtypeStruct(shape, BF16)


CORES = 2
MESH = pl.DeviceIdType.MESH
ANY = pl.BlockSpec(memory_space=pl.ANY)


class Ring:
    def __init__(self, n):
        self.n, self.chips = n, n // CORES
        self.long = self.chips // 2
        self.short = self.chips - 1 - self.long
        me = lax.axis_index("dp")
        self.me, self.z, self.core = me, lax.div(me, CORES), lax.rem(me, CORES)
        self.other = self.at(self.z, 1 - self.core)

    def chip(self, away):
        return lax.rem(self.z + away + self.chips, self.chips)

    def at(self, z, core):
        return z * CORES + core

    def to(self, away):
        return self.at(self.chip(away), self.core)

    def meet(self):
        barrier = pltpu.get_barrier_semaphore()
        for device in (self.to(1), self.to(-1), self.other):
            pl.semaphore_signal(barrier, inc=1, device_id={"dp": device}, device_id_type=MESH)
        pl.semaphore_wait(barrier, 3)


def _send(src, dst, send, recv, device):
    return pltpu.make_async_remote_copy(src_ref=src, dst_ref=dst, send_sem=send, recv_sem=recv, device_id={"dp": device}, device_id_type=MESH)


class Gather:
    @staticmethod
    def scratch(n, count):
        dma, chips = pltpu.SemaphoreType.DMA, n // CORES
        return [dma((count, chips - 1)), dma((count, chips - 1)), dma((count, chips)), dma((count, chips)), dma((count,))]

    def __init__(self, n, groups, sems):
        self.ring, self.groups = Ring(n), groups
        self.ring_send, self.ring_recv, self.pair_send, self.pair_recv, self.own = sems
        self.events = len(groups) * self.ring.long
        self.index = {}
        for number, group in enumerate(groups):
            for entry in range(len(group)):
                self.index[number, entry] = len(self.index)

    def place(self, item, owner):
        block, whole, column = item
        rows, cols = block.shape
        return whole.at[pl.ds(pl.multiple_of(owner * rows, rows), rows), pl.ds(column, cols)]

    def hop(self, x, item, slot, owner, device, first=False):
        place = self.place(item, owner)
        return _send(item[0] if first else place, place, self.ring_send.at[x, slot], self.ring_recv.at[x, slot], device)

    def pair(self, x, item, slot, owner, first=False):
        place = self.place(item, owner)
        return _send(item[0] if first else place, place, self.pair_send.at[x, slot], self.pair_recv.at[x, slot], self.ring.other)

    def each(self):
        for number, group in enumerate(self.groups):
            for entry, item in enumerate(group):
                yield self.index[number, entry], item, 1 - 2 * (number % 2)

    def start(self):
        r = self.ring
        r.meet()
        for x, item, way in self.each():
            self.hop(x, item, 0, r.me, r.to(way), True).start()
            self.hop(x, item, r.long, r.me, r.to(-way), True).start()
            self.pair(x, item, 0, r.me, True).start()
            pltpu.make_async_copy(item[0], self.place(item, r.me), self.own.at[x]).start()

    def event(self, k):
        r = self.ring
        t = lax.div(k, len(self.groups)) + 1
        for number, group in enumerate(self.groups):

            @pl.when(lax.rem(k, len(self.groups)) == number)
            def _():
                way = 1 - 2 * (number % 2)
                for entry, item in enumerate(group):
                    x = self.index[number, entry]
                    owner = r.to(-way * t)
                    self.hop(x, item, t - 1, owner, r.to(way)).wait_recv()

                    @pl.when(t < r.long)
                    def _():
                        self.hop(x, item, t, owner, r.to(way)).start()

                    self.pair(x, item, t, owner).start()

                    @pl.when(t <= r.short)
                    def _():
                        owner = r.to(way * t)
                        self.hop(x, item, r.long + t - 1, owner, r.to(-way)).wait_recv()

                        @pl.when(t < r.short)
                        def _():
                            self.hop(x, item, r.long + t, owner, r.to(-way)).start()

                        self.pair(x, item, r.long + t, owner).start()

    def finish(self):
        r = self.ring
        for x, item, way in self.each():
            pltpu.make_async_copy(item[0], self.place(item, r.me), self.own.at[x]).wait()
            for slot in range(r.chips - 1):
                self.hop(x, item, slot, r.me, r.to(1)).wait_send()
            for slot in range(r.chips):
                away = -way * slot if slot <= r.long else way * (slot - r.long)
                self.pair(x, item, slot, r.me).wait_send()
                self.pair(x, item, slot, r.at(r.chip(away), 1 - r.core)).wait_recv()


class Scatter:
    @staticmethod
    def scratch(n, rows, cols, pieces):
        dma, chips = pltpu.SemaphoreType.DMA, n // CORES
        return [pltpu.VMEM((chips, rows, cols), BF16), pltpu.VMEM((chips, rows, cols), BF16), pltpu.VMEM((chips - 1, rows, cols), BF16),
                dma((pieces,)), dma((pieces,)), dma((pieces,)), dma((pieces, chips - 1)), dma((pieces, chips - 1))]

    def __init__(self, n, mine, out, pieces, scratch):
        self.ring, self.mine, self.out, self.pieces = Ring(n), mine, out, pieces
        self.own, self.sum, self.got, self.own_sem, self.pair_send, self.pair_recv, self.ring_send, self.ring_recv = scratch
        self.events = pieces * (self.ring.long + 1)
        self.size = out.shape[0] // pieces

    def rows(self, a):
        return pl.ds(pl.multiple_of(a * self.size, self.size), self.size)

    def pair(self, a):
        return _send(self.mine.at[1 - self.ring.core, :, self.rows(a), :], self.sum.at[:, self.rows(a), :], self.pair_send.at[a], self.pair_recv.at[a],
                     self.ring.other)

    def own_copy(self, a):
        return pltpu.make_async_copy(self.mine.at[self.ring.core, :, self.rows(a), :], self.own.at[:, self.rows(a), :], self.own_sem.at[a])

    def hop(self, a, slot, chip, device):
        return _send(self.sum.at[chip, self.rows(a), :], self.got.at[slot, self.rows(a), :], self.ring_send.at[a, slot], self.ring_recv.at[a, slot], device)

    def start(self, meet=True):
        if meet:
            self.ring.meet()
        for a in range(self.pieces):
            self.pair(a).start()
            self.own_copy(a).start()

    def here(self, a, chip):
        return self.own[chip, self.rows(a), :].astype(F32) + self.sum[chip, self.rows(a), :].astype(F32)

    def add(self, a, slot):
        return self.got[slot, self.rows(a), :].astype(F32)

    def put(self, a, slot, chip, device, value):
        self.sum[chip, self.rows(a), :] = value.astype(BF16)
        self.hop(a, slot, chip, device).start()

    def event(self, k):
        r = self.ring
        t, a = lax.div(k, self.pieces), lax.rem(k, self.pieces)
        way = 1 - 2 * lax.rem(a, 2)
        far, near = r.chip(way * (r.long - t)), r.chip(-way * (r.short - t))

        @pl.when(t == 0)
        def _():
            self.own_copy(a).wait()
            self.pair(a).wait_recv()
            self.put(a, 0, far, r.to(way), self.here(a, far))
            self.put(a, r.long, near, r.to(-way), self.here(a, near))

        @pl.when((t > 0) & (t < r.long))
        def _():
            self.hop(a, t - 1, far, r.to(way)).wait_recv()
            self.put(a, t, far, r.to(way), self.here(a, far) + self.add(a, t - 1))

        @pl.when((t > 0) & (t < r.short))
        def _():
            self.hop(a, r.long + t - 1, near, r.to(-way)).wait_recv()
            self.put(a, r.long + t, near, r.to(-way), self.here(a, near) + self.add(a, r.long + t - 1))

        @pl.when(t == r.long)
        def _():
            one, two = r.long - 1, r.chips - 2
            self.hop(a, one, r.z, r.to(way)).wait_recv()
            self.hop(a, two, r.z, r.to(-way)).wait_recv()
            self.out[self.rows(a), :] = (self.here(a, r.z) + (self.add(a, one) + self.add(a, two))).astype(BF16)

    def finish(self):
        r = self.ring
        for a in range(self.pieces):
            self.pair(a).wait_send()
            for slot in range(r.chips - 1):
                self.hop(a, slot, r.z, r.to(1)).wait_send()


def _events(side, site, first, per):
    upto = lambda s: jnp.clip((s - first) * per, 0, side.events)
    lax.fori_loop(upto(site), upto(site + 1), lambda k, _: side.event(k), None)


def _rest(side, sites, first, per):
    done = min(max((sites - first) * per, 0), side.events)
    lax.fori_loop(done, side.events, lambda k, _: side.event(k), None)
    side.finish()


def _qkv_kernel(h_ref, w_ref, c_ref, s_ref, q_ref, k_ref, v_ref):
    heads = q_ref.shape[0]
    a = _normed(h_ref[...].astype(F32))
    r = _dot(a, w_ref[:, : (heads + 2) * HEAD], 1, 0).astype(BF16)
    c, s = c_ref[...], s_ref[...]
    for n in range(heads + 1):
        t = r[:, n * HEAD : (n + 1) * HEAD].astype(F32)
        t = (t * c + pltpu.roll(t, HEAD // 2, 1) * s).astype(BF16)
        if n < heads:
            q_ref[n] = t
        else:
            k_ref[...] = t
    v_ref[...] = r[:, (heads + 1) * HEAD :]


def qkv(h, w, c, s, heads, bt=512):
    t, d = h.shape
    bt = min(bt, t)
    cols = (heads + 2) * HEAD
    return _call(
        _qkv_kernel, (t // bt,),
        [_rows(bt, d), _whole(*w.shape), _rows(bt, HEAD), _rows(bt, HEAD)],
        [_heads(heads, bt, HEAD), _rows(bt, HEAD), _rows(bt, HEAD)],
        [_out(heads, t, HEAD), _out(t, HEAD), _out(t, HEAD)],
        flops=2 * t * d * cols, size=2 * (t * d + w.size + t * cols) + 8 * t * HEAD,
    )(h, w, c, s)


def _gap(bk, cols, bq):
    return lax.rem(lax.broadcasted_iota(jnp.int32, (bk, cols), 1), bq) - lax.broadcasted_iota(jnp.int32, (bk, cols), 0)


def _attend_kernel(q_ref, k_ref, v_ref, h_ref, w_ref, wg_ref, wu_ref, wd_ref, o_ref, lse_ref, y_ref, wgu_out, wd_out, top_s, mix_s, gap_s, *sems,
                   bk, wide, n, layer, first, per, q_blocks):
    g, bq, d = q_ref.shape
    cols = g * bq
    iq = pl.program_id(0)
    scale = d**-0.5
    e = scale * LOG2E
    at_all = range(0, cols, wide)
    ones = jnp.ones((8, bk), BF16)
    f = wg_ref.shape[2]
    side = Gather(n, [[(wg_ref.at[layer], wgu_out, 0)], [(wu_ref.at[layer], wgu_out, f)], [(wd_ref.at[layer], wd_out, 0)]], sems)
    steps = pl.num_programs(0)

    @pl.when(iq == 0)
    def _():
        side.start()
        gap_s[...] = _gap(bk, cols, bq)

    top_s[...] = jnp.full_like(top_s, NEG)
    mix_s[...] = jnp.zeros_like(mix_s)

    def block(j, masked):
        here = pl.ds(pl.multiple_of(j * bk, bk), bk)
        qs = q_ref[...].reshape(cols, d)
        scores = [_dot(k_ref[here, :], qs[at : at + wide, :], 1, 1) for at in at_all]
        weights, keeps = [], []
        for at, s in zip(at_all, scores):
            if masked:
                s = jnp.where(gap_s[:, at : at + wide] >= j * bk - iq * bq, s, HIDDEN)
            old = top_s[:, at : at + wide]
            top = jnp.maximum(old, s.max(axis=0, keepdims=True))
            top_s[:, at : at + wide] = top
            weights.append(jnp.exp2((s - top) * e).astype(BF16))
            keeps.append(jnp.exp2((old - top) * e))
        values = jnp.concatenate([v_ref[here, :].T, ones], axis=0)
        for at, p, keep in zip(at_all, weights, keeps):
            mix_s[:, at : at + wide] = mix_s[:, at : at + wide] * keep + _dot(values, p, 1, 0)
        _events(side, lax.div(iq * (iq + 1), 2) + j, first, per)

    lax.fori_loop(0, iq, lambda j, _: block(j, False), None)
    block(iq, True)
    total = mix_s[d : d + 1, :]
    o = (mix_s[:d, :] * (1 / total)).astype(BF16)
    lse = top_s[...] * scale + jnp.log(total)
    for m in range(g):
        o_ref[:, m * d : (m + 1) * d] = o[:, m * bq : (m + 1) * bq].T
        lse_ref[m : m + 1, :] = lse[:, m * bq : (m + 1) * bq]
    out = _dot(o_ref[...], w_ref[:, w_ref.shape[1] - h_ref.shape[1] :], 1, 0).astype(BF16)
    y_ref[...] = (h_ref[...].astype(F32) + out.astype(F32)).astype(BF16)

    @pl.when(iq == steps - 1)
    def _():
        _rest(side, q_blocks * (q_blocks + 1) // 2, first, per)


def attend(q, k, v, h, w, wg, wu, wd, layer, n, comm, bq=512, wide=512, first=2, per=1):
    g, t, d = q.shape
    bq = bk = min(bq, t)
    width, f = h.shape[1], wg.shape[2]
    return _call(
        functools.partial(_attend_kernel, bk=bk, wide=wide, n=n, layer=layer, first=first, per=per, q_blocks=t // bq), (t // bq,),
        [_heads(g, bq, d), _whole(t, d), _whole(t, d), _rows(bq, width), _whole(*w.shape), ANY, ANY, ANY],
        [_rows(bq, g * d), pl.BlockSpec((g, bq), lambda i: (0, i)), _rows(bq, width), ANY, ANY],
        [_out(t, g * d), jax.ShapeDtypeStruct((g, t), F32), _out(t, width), _out(width, 2 * f), _out(f, width)],
        [pltpu.VMEM((1, g * bq), F32), pltpu.VMEM((d + 8, g * bq), F32), pltpu.VMEM((bk, g * bq), jnp.int32), *Gather.scratch(n, 3)],
        flops=2 * g * t * t * d + 2 * t * width * g * d, size=2 * t * (3 * g * d + 2 * width), exps=g * t * t // 2, comm=comm,
    )(q, k, v, h, w, wg, wu, wd)


def _attention_weights(refs, layer, whole):
    group, column = [], 0
    for ref in refs:
        group.append((ref.at[layer], whole, column))
        column += ref.shape[2]
    return [group]


def _ffn_kernel(h_ref, wgu_ref, wd_ref, wq_ref, wk_ref, wv_ref, wo_ref, y_ref, wa_out, *sems, bc, n, layer):
    f = wd_ref.shape[0]
    i, steps = pl.program_id(0), pl.num_programs(0)
    side = Gather(n, _attention_weights((wq_ref, wk_ref, wv_ref, wo_ref), layer, wa_out), sems)

    @pl.when(i == 0)
    def _():
        side.start()

    _events(side, i, 1, 1)
    wide = h_ref[...].astype(F32)
    b = _normed(wide)
    out = jnp.zeros(wide.shape, F32)
    for c in range(0, f, bc):
        gate = _dot(b, wgu_ref[:, c : c + bc], 1, 0)
        up = _dot(b, wgu_ref[:, f + c : f + c + bc], 1, 0)
        act = (gate * lax.logistic(gate) * up).astype(BF16)
        out += _dot(act, wd_ref[c : c + bc, :], 1, 0)
    y_ref[...] = (wide + out.astype(BF16).astype(F32)).astype(BF16)

    @pl.when(i == steps - 1)
    def _():
        _rest(side, FFN_STEPS, 1, 1)


FFN_STEPS = 4


def ffn(h, wgu, wd, blocks, layer, n, comm, bc=512):
    t, d = h.shape
    bt = t // FFN_STEPS
    return _call(
        functools.partial(_ffn_kernel, bc=bc, n=n, layer=layer), (FFN_STEPS,),
        [_rows(bt, d), _whole(*wgu.shape), _whole(*wd.shape)] + [ANY] * 4, [_rows(bt, d), ANY],
        [_out(t, d), _out(d, sum(w.shape[2] for w in blocks))], Gather.scratch(n, 4),
        flops=2 * t * (wgu.size + wd.size), size=2 * (2 * t * d + wgu.size + wd.size), exps=t * wd.shape[0], comm=comm,
    )(h, wgu, wd, *blocks)


def _first_kernel(wq_ref, wk_ref, wv_ref, wo_ref, wa_out, *sems, n):
    side = Gather(n, _attention_weights((wq_ref, wk_ref, wv_ref, wo_ref), 0, wa_out), sems)
    side.start()
    _rest(side, 0, 0, 1)


def fetched(blocks, d, n, comm):
    return _call(functools.partial(_first_kernel, n=n), (), [ANY] * 4, ANY, _out(d, sum(w.shape[2] for w in blocks)), Gather.scratch(n, 4),
                 comm=comm)(*blocks)


def _ffn_back_kernel(by_ref, h_ref, o_ref, wgu_ref, wd_ref, wa_ref, *rest, bc, n, carries):
    if carries:
        mine_ref, dy_ref, do_ref, delta_ref, gw_ref, sum_ref, agu, ad, ao, *scratch = rest
        side = Scatter(n, mine_ref, sum_ref, CARRIED, scratch)
    else:
        dy_ref, do_ref, delta_ref, gw_ref, agu, ad, ao = rest
    i, last = pl.program_id(0), pl.num_programs(0) - 1
    f, d = wd_ref.shape
    g = do_ref.shape[0]
    bt = by_ref.shape[0]

    @pl.when(i == 0)
    def _():
        if carries:
            side.start()
        agu[...] = jnp.zeros_like(agu)
        ad[...] = jnp.zeros_like(ad)
        ao[...] = jnp.zeros_like(ao)

    if carries:
        _events(side, i, 0, CARRIED)
    by = by_ref[...]
    wide = h_ref[...].astype(F32)
    b = _normed(wide)
    bT, byT = b.T, by.T
    db = jnp.zeros((bt, d), F32)
    for c in range(0, f, bc):
        gate = _dot(b, wgu_ref[:, c : c + bc], 1, 0)
        up = _dot(b, wgu_ref[:, f + c : f + c + bc], 1, 0)
        da = _dot(by, wd_ref[c : c + bc, :], 1, 1).astype(BF16).astype(F32)
        sig = lax.logistic(gate)
        silu = gate * sig
        act = (silu * up).astype(BF16)
        dup = (da * silu).astype(BF16)
        dgate = (da * up * (sig + silu * (1 - sig))).astype(BF16)
        ad[:, c : c + bc] += _dot(byT, act, 1, 0)
        agu[:, c : c + bc] += _dot(bT, dgate, 1, 0)
        agu[:, f + c : f + c + bc] += _dot(bT, dup, 1, 0)
        db += _dot(dgate, wgu_ref[:, c : c + bc], 1, 1) + _dot(dup, wgu_ref[:, f + c : f + c + bc], 1, 1)
    dy = _norm_back(wide, db, by.astype(F32))
    dy_ref[...] = dy
    o = o_ref[...]
    do = _dot(dy, wa_ref[:, wa_ref.shape[1] - d :], 1, 1).astype(BF16)
    ao[...] += _dot(o.T, dy, 1, 0)
    prod = do.astype(F32) * o.astype(F32)
    lane = lax.broadcasted_iota(jnp.int32, (bt, HEAD), 1)
    deltas = jnp.zeros((bt, HEAD), F32)
    for m in range(g):
        do_ref[m] = do[:, m * HEAD : (m + 1) * HEAD]
        deltas = jnp.where(lane == m, prod[:, m * HEAD : (m + 1) * HEAD].sum(-1, keepdims=True), deltas)
    delta_ref[...] = deltas.T[:g, :]

    @pl.when(i == last)
    def _():
        down, r, rd = ad[...].astype(BF16).T, d // n, f // n
        for owner in range(n):
            mine = gw_ref.at[owner % CORES, owner // CORES]
            top = 0
            for c in range(0, 2 * f, d):
                mine[top : top + r, :] = agu[owner * r : (owner + 1) * r, c : c + d].astype(BF16)
                top += r
            mine[top : top + rd, :] = down[owner * rd : (owner + 1) * rd, :]
            ro = ao.shape[0] // n
            mine[top + rd : top + rd + ro, :] = ao[owner * ro : (owner + 1) * ro, :].astype(BF16)
        if carries:
            _rest(side, BACK_STEPS, 0, CARRIED)


BACK_STEPS = 4
CARRIED = 1


def ffn_back(by, h, o, wgu, wd, wa, n, mine=None, comm=None, bc=512):
    t, d = h.shape
    bt = t // BACK_STEPS
    f = wd.shape[0]
    carries = mine is not None
    rows = (2 * d * f + f * d + o.shape[1] * d) // n // d
    g = o.shape[1] // HEAD
    return _call(
        functools.partial(_ffn_back_kernel, bc=bc, n=n, carries=carries), (BACK_STEPS,),
        [_rows(bt, d), _rows(bt, d), _rows(bt, g * HEAD), _whole(*wgu.shape), _whole(*wd.shape), _whole(*wa.shape)] + [ANY] * carries,
        [_rows(bt, d), _heads(g, bt, HEAD), pl.BlockSpec((g, bt), lambda i: (0, i)), _whole(CORES, n // CORES, rows, d)]
        + ([_whole(*mine.shape[2:])] if carries else []),
        [_out(t, d), _out(g, t, HEAD), jax.ShapeDtypeStruct((g, t), F32), _out(CORES, n // CORES, rows, d)]
        + ([_out(*mine.shape[2:])] if carries else []),
        [pltpu.VMEM((d, 2 * f), F32), pltpu.VMEM((d, f), F32), pltpu.VMEM((g * HEAD, d), F32)]
        + (Scatter.scratch(n, *mine.shape[2:], CARRIED) if carries else []),
        flops=2 * t * d * (8 * f + 2 * g * HEAD), size=2 * (5 * t * d + 2 * wgu.size + 2 * wd.size + wa.size), exps=t * f, comm=comm,
    )(by, h, o, wgu, wd, wa, *([mine] if carries else []))


def _attend_back_kernel(q_ref, k_ref, v_ref, do_ref, lse_ref, delta_ref, mine_ref, dq_ref, dk_ref, dv_ref, sum_ref, dq_s, dk_s, dv_s, gap_s, *scratch,
                        bk, wide, n, q_blocks, first, per):
    g, bq, d = q_ref.shape
    cols = g * bq
    iq = pl.program_id(0)
    scale = d**-0.5
    e = scale * LOG2E
    at_all = range(0, cols, wide)

    side = Scatter(n, mine_ref, sum_ref, PIECES, scratch)

    @pl.when(iq == 0)
    def _():
        side.start()
        gap_s[...] = _gap(bk, cols, bq)
        dk_s[...] = jnp.zeros_like(dk_s)
        dv_s[...] = jnp.zeros_like(dv_s)

    dq_s[...] = jnp.zeros_like(dq_s)
    lse = jnp.concatenate([lse_ref[m : m + 1, :] for m in range(g)], axis=1) * LOG2E
    delta = jnp.concatenate([delta_ref[m : m + 1, :] for m in range(g)], axis=1)

    def block(j, masked):
        here = pl.ds(pl.multiple_of(j * bk, bk), bk)
        qs = [q_ref[...].reshape(cols, d)[at : at + wide, :] for at in at_all]
        dos = [do_ref[...].reshape(cols, d)[at : at + wide, :] for at in at_all]
        scores = [_dot(k_ref[here, :], x, 1, 1) for x in qs]
        dps = [_dot(v_ref[here, :], x, 1, 1) for x in dos]
        for m, at in enumerate(at_all):
            p = jnp.exp2(scores[m] * e - lse[:, at : at + wide])
            if masked:
                p = jnp.where(gap_s[:, at : at + wide] >= j * bk - iq * bq, p, 0.0)
            ds = (p * (dps[m] - delta[:, at : at + wide])).astype(BF16)
            dv_s[here, :] += _dot(p.astype(BF16), dos[m], 1, 0)
            dk_s[here, :] += _dot(ds, qs[m], 1, 0)
            dq_s[:, at : at + wide] += _dot(k_ref[here, :].T, ds, 1, 0)
        _events(side, lax.div(iq * (iq + 1), 2) + j, first, per)

    lax.fori_loop(0, iq, lambda j, _: block(j, False), None)
    block(iq, True)
    dq_ref[...] = (dq_s[...] * scale).astype(BF16).T.reshape(g, bq, d)

    @pl.when(iq == pl.num_programs(0) - 1)
    def _():
        dk_ref[...] = (dk_s[...] * scale).astype(BF16)
        dv_ref[...] = dv_s[...].astype(BF16)
        _rest(side, q_blocks * (q_blocks + 1) // 2, first, per)


PIECES = 4


def attend_back(q, k, v, do, lse, delta, mine, n, comm, bq=512, wide=512, first=1, per=2):
    g, t, d = q.shape
    bq = bk = min(bq, t)
    stats = pl.BlockSpec((g, bq), lambda i: (0, i))
    return _call(
        functools.partial(_attend_back_kernel, bk=bk, wide=wide, n=n, q_blocks=t // bq, first=first, per=per), (t // bq,),
        [_heads(g, bq, d), _whole(t, d), _whole(t, d), _heads(g, bq, d), stats, stats, ANY],
        [_heads(g, bq, d), _whole(t, d), _whole(t, d), _whole(*mine.shape[2:])],
        [_out(g, t, d), _out(t, d), _out(t, d), _out(*mine.shape[2:])],
        [pltpu.VMEM((d, g * bq), F32), pltpu.VMEM((t, d), F32), pltpu.VMEM((t, d), F32), pltpu.VMEM((bk, g * bq), jnp.int32),
         *Scatter.scratch(n, *mine.shape[2:], PIECES)],
        flops=5 * g * t * t * d, size=2 * t * d * (3 * g + 4), exps=g * t * t // 2, comm=comm,
    )(q, k, v, do, lse, delta, mine)


def _qkv_back_kernel(dq_ref, dk_ref, dv_ref, h_ref, c_ref, s_ref, w_ref, *rest, onward, n):
    i, last = pl.program_id(0), pl.num_programs(0) - 1
    by_ref, dy_ref = (rest[0], rest[1]) if onward else (None, None)
    gw_ref, acc = rest[-2:]
    heads = dq_ref.shape[0]

    @pl.when(i == 0)
    def _():
        acc[...] = jnp.zeros_like(acc)

    c, s = c_ref[...], s_ref[...]
    parts = []
    for m in range(heads + 1):
        t = (dq_ref[m] if m < heads else dk_ref[...]).astype(F32)
        parts.append((t * c - pltpu.roll(t, HEAD // 2, 1) * s).astype(BF16))
    by_qkv = jnp.concatenate(parts + [dv_ref[...]], axis=1)
    wide = h_ref[...].astype(F32)
    a = _normed(wide)
    acc[...] += _dot(a.T, by_qkv, 1, 0)
    if onward:
        da = _dot(by_qkv, w_ref[:, : by_qkv.shape[1]], 1, 1)
        dy_ref[...] = _norm_back(wide, da, by_ref[...].astype(F32))

    @pl.when(i == last)
    def _():
        d, width = wide.shape[1], heads * HEAD
        r = d // n
        for owner in range(n):
            mine = gw_ref.at[owner % CORES, owner // CORES]
            at = owner * r
            mine[:r, :] = acc[at : at + r, :width].astype(BF16)
            mine[r:, : 2 * HEAD] = acc[at : at + r // 2, width:].astype(BF16)
            mine[r:, 2 * HEAD :] = acc[at + r // 2 : at + r, width:].astype(BF16)


def qkv_back(dq, dk, dv, h, c, s, w, by, n, bt=512):
    heads, t, _ = dq.shape
    d = h.shape[1]
    bt = min(bt, t)
    cols = (heads + 2) * HEAD
    onward = by is not None
    shape = (CORES, n // CORES, 3 * d // n // 2, heads * HEAD)
    got = _call(
        functools.partial(_qkv_back_kernel, onward=onward, n=n), (t // bt,),
        [_heads(heads, bt, HEAD), _rows(bt, HEAD), _rows(bt, HEAD), _rows(bt, d), _rows(bt, HEAD), _rows(bt, HEAD), _whole(*w.shape)]
        + [_rows(bt, d)] * onward,
        [_rows(bt, d)] * onward + [_whole(*shape)],
        [_out(t, d)] * onward + [_out(*shape)],
        [pltpu.VMEM((d, cols), F32)],
        flops=2 * t * d * cols * (2 if onward else 1), size=2 * t * (cols + 3 * d), exps=0,
    )(dq, dk, dv, h, c, s, w, *([by] if onward else []))
    return got[-1], got[0] if onward else None


def tables(t):
    half = HEAD // 2
    angle = jnp.arange(t, dtype=F32)[:, None] * THETA ** (-jnp.arange(half, dtype=F32) / half)
    cos, sin = jnp.cos(angle), jnp.sin(angle)
    return jnp.concatenate([cos, cos], -1), jnp.concatenate([-sin, sin], -1)


def _last_kernel(mine_ref, *rest, n, given, pieces):
    refs, (sum_ref, all_ref, box, square_send, square_recv), scratch = rest[:given], rest[given : given + 5], rest[given + 5 :]
    side = Scatter(n, mine_ref, sum_ref, pieces, scratch)
    r = side.ring
    me = r.me
    barrier = pltpu.get_barrier_semaphore()
    away = lambda i: lax.rem(me + i, n)
    for i in range(1, n):
        pl.semaphore_signal(barrier, inc=1, device_id={"dp": away(i)}, device_id_type=MESH)
    pl.semaphore_wait(barrier, n - 1)
    side.start(meet=False)
    square = lambda ref: jnp.sum(ref[...].astype(F32) ** 2)
    total = sum(square(ref) for ref in refs)
    lax.fori_loop(0, side.events, lambda k, _: side.event(k), None)
    box[me] = jnp.full(box.shape[1:], total + square(sum_ref), F32)
    post = lambda i: _send(box.at[me], box.at[me], square_send.at[i], square_recv.at[me], away(i))
    for i in range(1, n):
        post(i).start()
    for i in range(1, n):
        _send(box.at[away(i)], box.at[away(i)], square_send.at[i], square_recv.at[away(i)], away(i)).wait_recv()
    whole = box[0]
    for i in range(1, n):
        whole = whole + box[i]
    all_ref[...] = whole
    for i in range(1, n):
        post(i).wait_send()
    side.finish()


def last(mine, sums, n, comm, pieces=3):
    rows, cols = mine.shape[2:]
    tile = (8, 128)
    dma = pltpu.SemaphoreType.DMA
    vmem = pl.BlockSpec(memory_space=pltpu.VMEM)
    return _call(
        functools.partial(_last_kernel, n=n, given=len(sums), pieces=pieces), (), [ANY] + [vmem] * len(sums), [vmem, vmem],
        [_out(rows, cols), jax.ShapeDtypeStruct(tile, F32)],
        [pltpu.VMEM((n, *tile), F32), dma((n,)), dma((n,)), *Scatter.scratch(n, rows, cols, pieces)], comm=comm,
    )(mine, *sums)


def _adamw_kernel(*refs, layers, count):
    sums, (square,), refs = refs[: 2 * layers], refs[2 * layers : 2 * layers + 1], refs[2 * layers + 1 :]
    weights, ms, vs, new_w, new_m, new_v = (refs[i : i + 7] for i in range(0, 42, 7))
    factor = jnp.minimum(1.0, 0.5 * lax.rsqrt(square[:1, :1] / count + 1e-30))

    def take(which, layer, rows, cols, g):
        g = g.astype(F32) * factor
        at = (layer, rows, cols)
        m = 0.9 * ms[which][at] + 0.1 * g
        v = 0.95 * vs[which][at] + 0.05 * g * g
        w = weights[which][at].astype(F32)
        new_w[which][at] = (w - 0.02 * (m * lax.rsqrt(v + 1e-8) + 0.1 * w)).astype(BF16)
        new_m[which][at], new_v[which][at] = m, v

    whole = slice(None)
    for layer in range(layers):
        qkv, rest = sums[2 * layer], sums[2 * layer + 1]
        r, d = weights[0].shape[1], rest.shape[1]
        take(0, layer, whole, whole, qkv[:r, :])
        for half in range(2):
            rows = slice(half * (r // 2), (half + 1) * (r // 2))
            for which in range(2):
                at = (2 * half + which) * HEAD
                take(1 + which, layer, rows, whole, qkv[r:, at : at + HEAD])
        top = 0
        for which in (4, 5):
            for c in range(0, weights[which].shape[2], d):
                take(which, layer, whole, slice(c, c + d), rest[top : top + r, :])
                top += r
        for which in (6, 3):
            size = weights[which].shape[1]
            take(which, layer, whole, whole, rest[top : top + size, :])
            top += size


def adamw(sums, square, weights, m, v, n):
    layers = weights[0].shape[0]
    vmem = pl.BlockSpec(memory_space=pltpu.VMEM)
    count = n * sum(w.size for w in weights)
    return _call(
        functools.partial(_adamw_kernel, layers=layers, count=float(count)), (), [vmem] * (2 * layers + 22), [vmem] * 21,
        [jax.ShapeDtypeStruct(a.shape, a.dtype) for a in (*weights, *m, *v)],
    )(*sums, square, *weights, *m, *v)


def solution(mesh):
    def step(x, dy, *arrays):
        weights, m, v = (arrays[i : i + 7] for i in (0, 7, 14))
        wq, wk, wv, wo, wg, wu, wd = weights
        layers, n = wq.shape[0], mesh.shape["dp"]
        heads = wo.shape[1] * n // HEAD
        ids = iter(range(1, 100))
        c, s = tables(x.shape[1])
        h, kept = x[0], []
        wa = fetched((wq, wk, wv, wo), x.shape[2], n, next(ids))
        for layer in range(layers):
            q, k, val = qkv(h, wa, c, s, heads)
            o, lse, h1, wgu, wdn = attend(q, k, val, h, wa, wg, wu, wd, layer, n, next(ids))
            kept.append((h, q, k, val, o, lse, h1, wa, wgu, wdn))
            if layer < layers - 1:
                h, wa = ffn(h1, wgu, wdn, (wq, wk, wv, wo), layer + 1, n, next(ids))
        by, sums, mine = dy[0], [None] * (2 * layers), None
        for layer in reversed(range(layers)):
            h, q, k, val, o, lse, h1, wa, wgu, wdn = kept[layer]
            if mine is None:
                by, do, delta, rest = ffn_back(by, h1, o, wgu, wdn, wa, n)
            else:
                by, do, delta, rest, sums[2 * layer + 2] = ffn_back(by, h1, o, wgu, wdn, wa, n, mine, next(ids))
            dq, dk, dv, sums[2 * layer + 1] = attend_back(q, k, val, do, lse, delta, rest, n, next(ids))
            mine, by = qkv_back(dq, dk, dv, h, c, s, wa, by if layer else None, n)
        sums[0], square = last(mine, sums[1:], n, next(ids))
        return tuple(adamw(sums, square, weights, m, v, n))

    states, cut = P(("rep", "dp"), None, None), P(None, "dp", None)
    return jax.shard_map(
        step,
        mesh=mesh,
        in_specs=(states, states) + (cut,) * 21,
        out_specs=(P("rep", "dp", None),) * 21,
        check_vma=False,
    )
```

```python
import functools

import jax
import jax.numpy as jnp
from jax import lax
from jax.experimental import pallas as pl
from jax.experimental.pallas import tpu as pltpu
from jax.sharding import PartitionSpec as P

HEAD = 128
THETA = 10000
NEG = -1e30
HIDDEN = 2 * NEG
LOG2E = 1.4426950408889634
VMEM = 60 * 2**20
NAMES = ("wq", "wk", "wv", "wo", "w_gate", "w_up", "w_down")
F32, BF16 = jnp.float32, jnp.bfloat16


def _dot(a, b, ca, cb):
    return lax.dot_general(a, b, (((ca,), (cb,)), ((), ())), preferred_element_type=F32)


def _scale(wide):
    return lax.rsqrt(jnp.mean(wide * wide, -1, keepdims=True) + 1e-6)


def _normed(wide):
    return (wide * _scale(wide)).astype(BF16)


def _norm_back(wide, by, by_out):
    by = by.astype(BF16).astype(F32)
    s = _scale(wide)
    inner = s * by - wide * (s * s * s * jnp.mean(wide * by, -1, keepdims=True))
    return (by_out + inner.astype(BF16).astype(F32)).astype(BF16)


def _call(body, grid, ins, outs, shapes, scratch=(), flops=0, size=0, exps=0, comm=None):
    return pl.pallas_call(
        body,
        grid=grid,
        in_specs=ins,
        out_specs=outs,
        out_shape=shapes,
        scratch_shapes=list(scratch),
        compiler_params=pltpu.CompilerParams(dimension_semantics=("arbitrary",) * len(grid), vmem_limit_bytes=VMEM, collective_id=comm,
                                             has_side_effects=comm is not None),
        cost_estimate=pl.CostEstimate(flops=flops, bytes_accessed=size, transcendentals=exps),
    )


def _whole(*shape):
    return pl.BlockSpec(shape, lambda i: (0,) * len(shape), pipeline_mode=pl.Buffered(1))


def _rows(n, *rest):
    return pl.BlockSpec((n, *rest), lambda i: (i,) + (0,) * len(rest))


def _heads(h, n, *rest):
    return pl.BlockSpec((h, n, *rest), lambda i: (0, i) + (0,) * len(rest))


def _out(*shape):
    return jax.ShapeDtypeStruct(shape, BF16)


CORES = 2
MESH = pl.DeviceIdType.MESH
ANY = pl.BlockSpec(memory_space=pl.ANY)


class Ring:
    def __init__(self, n):
        self.n, self.chips = n, n // CORES
        self.long = self.chips // 2
        self.short = self.chips - 1 - self.long
        me = lax.axis_index("dp")
        self.me, self.z, self.core = me, lax.div(me, CORES), lax.rem(me, CORES)
        self.other = self.at(self.z, 1 - self.core)

    def chip(self, away):
        return lax.rem(self.z + away + self.chips, self.chips)

    def at(self, z, core):
        return z * CORES + core

    def to(self, away):
        return self.at(self.chip(away), self.core)

    def meet(self, reach=1):
        barrier = pltpu.get_barrier_semaphore()
        for device in (self.other, *(self.to(sign * i) for i in range(1, reach + 1) for sign in (1, -1))):
            pl.semaphore_signal(barrier, inc=1, device_id={"dp": device}, device_id_type=MESH)
        pl.semaphore_wait(barrier, 1 + 2 * reach)


def _send(src, dst, send, recv, device):
    return pltpu.make_async_remote_copy(src_ref=src, dst_ref=dst, send_sem=send, recv_sem=recv, device_id={"dp": device}, device_id_type=MESH)


class Gather:
    @staticmethod
    def scratch(n, count):
        dma, chips = pltpu.SemaphoreType.DMA, n // CORES
        return [dma((count, chips - 1)), dma((count, chips - 1)), dma((count, chips)), dma((count, chips)), dma((count,))]

    def __init__(self, n, groups, sems, reach=1):
        self.ring, self.groups, self.reach = Ring(n), groups, reach
        self.ring_send, self.ring_recv, self.pair_send, self.pair_recv, self.own = sems
        self.events = len(groups) * self.ring.long
        self.index = {}
        for number, group in enumerate(groups):
            for entry in range(len(group)):
                self.index[number, entry] = len(self.index)

    def place(self, item, owner):
        block, whole, column = item
        rows, cols = block.shape
        return whole.at[pl.ds(pl.multiple_of(owner * rows, rows), rows), pl.ds(column, cols)]

    def hop(self, x, item, slot, owner, device, first=False):
        place = self.place(item, owner)
        return _send(item[0] if first else place, place, self.ring_send.at[x, slot], self.ring_recv.at[x, slot], device)

    def pair(self, x, item, slot, owner, first=False):
        place = self.place(item, owner)
        return _send(item[0] if first else place, place, self.pair_send.at[x, slot], self.pair_recv.at[x, slot], self.ring.other)

    def each(self):
        for number, group in enumerate(self.groups):
            for entry, item in enumerate(group):
                yield self.index[number, entry], item, 1 - 2 * (number % 2)

    def start(self):
        r = self.ring
        r.meet(self.reach)
        for x, item, way in self.each():
            for i in range(self.reach):
                self.hop(x, item, i, r.me, r.to(way * (i + 1)), True).start()
                self.hop(x, item, r.long + i, r.me, r.to(-way * (i + 1)), True).start()
            self.pair(x, item, 0, r.me, True).start()
            pltpu.make_async_copy(item[0], self.place(item, r.me), self.own.at[x]).start()

    def event(self, k):
        r = self.ring
        t = lax.div(k, len(self.groups)) + 1
        for number, group in enumerate(self.groups):

            @pl.when(lax.rem(k, len(self.groups)) == number)
            def _():
                way = 1 - 2 * (number % 2)
                for entry, item in enumerate(group):
                    x = self.index[number, entry]
                    owner = r.to(-way * t)
                    self.hop(x, item, t - 1, owner, r.to(way)).wait_recv()

                    for i in range(self.reach):

                        @pl.when((lax.rem(t, self.reach) == 0) & (t + i < r.long))
                        def _():
                            self.hop(x, item, t + i, owner, r.to(way * (i + 1))).start()

                    self.pair(x, item, t, owner).start()

                    @pl.when(t <= r.short)
                    def _():
                        owner = r.to(way * t)
                        self.hop(x, item, r.long + t - 1, owner, r.to(-way)).wait_recv()

                        for i in range(self.reach):

                            @pl.when((lax.rem(t, self.reach) == 0) & (t + i < r.short))
                            def _():
                                self.hop(x, item, r.long + t + i, owner, r.to(-way * (i + 1))).start()

                        self.pair(x, item, r.long + t, owner).start()

    def finish(self):
        r = self.ring
        for x, item, way in self.each():
            pltpu.make_async_copy(item[0], self.place(item, r.me), self.own.at[x]).wait()

            def hop(slot, _):
                self.hop(x, item, slot, r.me, r.to(1)).wait_send()

            def pair(slot, _):
                away = jnp.where(slot <= r.long, -way * slot, way * (slot - r.long))
                self.pair(x, item, slot, r.me).wait_send()
                self.pair(x, item, slot, r.at(r.chip(away), 1 - r.core)).wait_recv()

            lax.fori_loop(0, r.chips - 1, hop, None)
            lax.fori_loop(0, r.chips, pair, None)


class Scatter:
    @staticmethod
    def scratch(n, rows, cols, pieces):
        dma, chips = pltpu.SemaphoreType.DMA, n // CORES
        return [pltpu.VMEM((chips, rows, cols), BF16), pltpu.VMEM((chips, rows, cols), BF16), pltpu.VMEM((chips - 1, rows, cols), BF16),
                dma((pieces,)), dma((pieces,)), dma((pieces,)), dma((pieces, chips - 1)), dma((pieces, chips - 1))]

    def __init__(self, n, mine, out, pieces, scratch):
        self.ring, self.mine, self.out, self.pieces = Ring(n), mine, out, pieces
        self.own, self.sum, self.got, self.own_sem, self.pair_send, self.pair_recv, self.ring_send, self.ring_recv = scratch
        self.events = pieces * (self.ring.long + 1)
        self.size = out.shape[0] // pieces

    def rows(self, a):
        return pl.ds(pl.multiple_of(a * self.size, self.size), self.size)

    def pair(self, a):
        return _send(self.mine.at[1 - self.ring.core, :, self.rows(a), :], self.sum.at[:, self.rows(a), :], self.pair_send.at[a], self.pair_recv.at[a],
                     self.ring.other)

    def own_copy(self, a):
        return pltpu.make_async_copy(self.mine.at[self.ring.core, :, self.rows(a), :], self.own.at[:, self.rows(a), :], self.own_sem.at[a])

    def hop(self, a, slot, chip, device):
        return _send(self.sum.at[chip, self.rows(a), :], self.got.at[slot, self.rows(a), :], self.ring_send.at[a, slot], self.ring_recv.at[a, slot], device)

    def start(self, meet=True):
        if meet:
            self.ring.meet()
        for a in range(self.pieces):
            self.pair(a).start()
            self.own_copy(a).start()

    def here(self, a, chip):
        return self.own[chip, self.rows(a), :].astype(F32) + self.sum[chip, self.rows(a), :].astype(F32)

    def add(self, a, slot):
        return self.got[slot, self.rows(a), :].astype(F32)

    def put(self, a, slot, chip, device, value):
        self.sum[chip, self.rows(a), :] = value.astype(BF16)
        self.hop(a, slot, chip, device).start()

    def event(self, k):
        r = self.ring
        t, a = lax.div(k, self.pieces), lax.rem(k, self.pieces)
        way = 1 - 2 * lax.rem(a, 2)
        far, near = r.chip(way * (r.long - t)), r.chip(-way * (r.short - t))

        @pl.when(t == 0)
        def _():
            self.own_copy(a).wait()
            self.pair(a).wait_recv()
            self.put(a, 0, far, r.to(way), self.here(a, far))
            self.put(a, r.long, near, r.to(-way), self.here(a, near))

        @pl.when((t > 0) & (t < r.long))
        def _():
            self.hop(a, t - 1, far, r.to(way)).wait_recv()
            self.put(a, t, far, r.to(way), self.here(a, far) + self.add(a, t - 1))

        @pl.when((t > 0) & (t < r.short))
        def _():
            self.hop(a, r.long + t - 1, near, r.to(-way)).wait_recv()
            self.put(a, r.long + t, near, r.to(-way), self.here(a, near) + self.add(a, r.long + t - 1))

        @pl.when(t == r.long)
        def _():
            one, two = r.long - 1, r.chips - 2
            self.hop(a, one, r.z, r.to(way)).wait_recv()
            self.hop(a, two, r.z, r.to(-way)).wait_recv()
            self.out[self.rows(a), :] = (self.here(a, r.z) + (self.add(a, one) + self.add(a, two))).astype(BF16)

    def finish(self):
        r = self.ring
        for a in range(self.pieces):
            self.pair(a).wait_send()
            lax.fori_loop(0, r.chips - 1, lambda slot, _: self.hop(a, slot, r.z, r.to(1)).wait_send(), None)


def _events(side, site, marks, per, last=None):
    upto = lambda at: jnp.minimum(per * sum((at > mark).astype(jnp.int32) for mark in marks), side.events)
    end = upto(site + 1) if last is None else jnp.where(last, side.events, upto(site + 1))
    lax.fori_loop(upto(site), end, lambda k, _: side.event(k), None)
    if last is not None:
        pl.when(last)(side.finish)


def _gap(bk, cols, bq):
    return lax.rem(lax.broadcasted_iota(jnp.int32, (bk, cols), 1), bq) - lax.broadcasted_iota(jnp.int32, (bk, cols), 0)


def _attend_kernel(h_ref, w_ref, c_ref, s_ref, wg_ref, wu_ref, wd_ref, q_ref, k_ref, v_ref, o_ref, lse_ref, y_ref, wgu_out, wd_out,
                   keys, values, top_s, mix_s, gap_s, *sems, wide, n, layer, marks):
    g, bq, d = q_ref.shape
    bk, cols = bq, g * bq
    iq, blocks = pl.program_id(0), keys.shape[0] // bq
    scale = d**-0.5
    e = scale * LOG2E
    at_all = range(0, cols, wide)
    f = wg_ref.shape[2]
    side = Gather(n, [[(wg_ref.at[layer], wgu_out, 0)], [(wu_ref.at[layer], wgu_out, f)], [(wd_ref.at[layer], wd_out, 0)]], sems)

    @pl.when(iq == 0)
    def _():
        side.start()
        gap_s[...] = _gap(bk, cols, bq)
        values[d:, :] = jnp.ones((8, values.shape[1]), BF16)

    mine = pl.ds(pl.multiple_of(iq * bq, bq), bq)
    r = _dot(_normed(h_ref[...].astype(F32)), w_ref[:, : (g + 2) * d], 1, 0).astype(BF16)
    c, s = c_ref[...], s_ref[...]
    for m in range(g + 1):
        t = r[:, m * d : (m + 1) * d].astype(F32)
        t = (t * c + pltpu.roll(t, d // 2, 1) * s).astype(BF16)
        if m < g:
            q_ref[m] = t
        else:
            k_ref[...] = t
            keys[mine, :] = t
    v = r[:, (g + 1) * d :]
    v_ref[...] = v
    values[:d, mine] = v.T
    top_s[...] = jnp.full_like(top_s, NEG)
    mix_s[...] = jnp.zeros_like(mix_s)

    site = lax.div(iq * (iq + 1), 2)

    def block(j, masked):
        here = pl.ds(pl.multiple_of(j * bk, bk), bk)
        qs = q_ref[...].reshape(cols, d)
        scores = [_dot(keys[here, :], qs[at : at + wide, :], 1, 1) for at in at_all]
        weights, keeps = [], []
        for at, s in zip(at_all, scores):
            if masked:
                s = jnp.where(gap_s[:, at : at + wide] >= 0, s, HIDDEN)
            old = top_s[:, at : at + wide]
            top = jnp.maximum(old, s.max(axis=0, keepdims=True))
            top_s[:, at : at + wide] = top
            weights.append(jnp.exp2((s - top) * e).astype(BF16))
            keeps.append(jnp.exp2((old - top) * e))
        for at, p, keep in zip(at_all, weights, keeps):
            mix_s[:, at : at + wide] = mix_s[:, at : at + wide] * keep + _dot(values[:, here], p, 1, 0)
        if not masked:
            _events(side, site + j, marks, 1)

    lax.fori_loop(0, iq, lambda j, _: block(j, False), None)
    block(iq, True)
    total = mix_s[d : d + 1, :]
    o = (mix_s[:d, :] * (1 / total)).astype(BF16)
    lse = top_s[...] * scale + jnp.log(total)
    for m in range(g):
        o_ref[:, m * d : (m + 1) * d] = o[:, m * bq : (m + 1) * bq].T
        lse_ref[m : m + 1, :] = lse[:, m * bq : (m + 1) * bq]
    out = _dot(o_ref[...], w_ref[:, w_ref.shape[1] - h_ref.shape[1] :], 1, 0).astype(BF16)
    y_ref[...] = (h_ref[...].astype(F32) + out.astype(F32)).astype(BF16)
    _events(side, site + iq, marks, 1, iq == blocks - 1)


def attend(h, w, c, s, wg, wu, wd, heads, layer, n, comm, bq=512, wide=512, marks=range(1, 10)):
    t, d = h.shape
    bq, g, f = min(bq, t), heads, wg.shape[2]
    return _call(
        functools.partial(_attend_kernel, wide=wide, n=n, layer=layer, marks=marks), (t // bq,),
        [_rows(bq, d), _whole(*w.shape), _rows(bq, HEAD), _rows(bq, HEAD), ANY, ANY, ANY],
        [_heads(g, bq, HEAD), _rows(bq, HEAD), _rows(bq, HEAD), _rows(bq, g * HEAD), pl.BlockSpec((g, bq), lambda i: (0, i)), _rows(bq, d), ANY, ANY],
        [_out(g, t, HEAD), _out(t, HEAD), _out(t, HEAD), _out(t, g * HEAD), jax.ShapeDtypeStruct((g, t), F32), _out(t, d), _out(d, 2 * f), _out(f, d)],
        [pltpu.VMEM((t, HEAD), BF16), pltpu.VMEM((HEAD + 8, t), BF16), pltpu.VMEM((1, g * bq), F32), pltpu.VMEM((HEAD + 8, g * bq), F32),
         pltpu.VMEM((bq, g * bq), jnp.int32), *Gather.scratch(n, 3)],
        flops=2 * g * t * t * HEAD + 2 * t * w.size, size=2 * t * (3 * g * HEAD + 2 * d), exps=g * t * t // 2, comm=comm,
    )(h, w, c, s, wg, wu, wd)


def _attention_weights(refs, layer, whole):
    group, column = [], 0
    for ref in refs:
        group.append((ref.at[layer], whole, column))
        column += ref.shape[2]
    return [group]


def _ffn_kernel(h_ref, wgu_ref, wd_ref, wq_ref, wk_ref, wv_ref, wo_ref, y_ref, wa_out, *sems, bc, n, layer):
    f = wd_ref.shape[0]
    i, steps = pl.program_id(0), pl.num_programs(0)
    side = Gather(n, _attention_weights((wq_ref, wk_ref, wv_ref, wo_ref), layer, wa_out), sems)

    @pl.when(i == 0)
    def _():
        side.start()

    wide = h_ref[...].astype(F32)
    b = _normed(wide)
    out = jnp.zeros(wide.shape, F32)
    for c in range(0, f, bc):
        gate = _dot(b, wgu_ref[:, c : c + bc], 1, 0)
        up = _dot(b, wgu_ref[:, f + c : f + c + bc], 1, 0)
        act = (gate * lax.logistic(gate) * up).astype(BF16)
        out += _dot(act, wd_ref[c : c + bc, :], 1, 0)
    y_ref[...] = (wide + out.astype(BF16).astype(F32)).astype(BF16)

    _events(side, i, range(FFN_STEPS), 1, i == steps - 1)


FFN_STEPS = 4


def ffn(h, wgu, wd, blocks, layer, n, comm, bc=512):
    t, d = h.shape
    bt = t // FFN_STEPS
    return _call(
        functools.partial(_ffn_kernel, bc=bc, n=n, layer=layer), (FFN_STEPS,),
        [_rows(bt, d), _whole(*wgu.shape), _whole(*wd.shape)] + [ANY] * 4, [_rows(bt, d), ANY],
        [_out(t, d), _out(d, sum(w.shape[2] for w in blocks))], Gather.scratch(n, 4),
        flops=2 * t * (wgu.size + wd.size), size=2 * (2 * t * d + wgu.size + wd.size), exps=t * wd.shape[0], comm=comm,
    )(h, wgu, wd, *blocks)


def _first_kernel(wq_ref, wk_ref, wv_ref, wo_ref, speed_ref, wa_out, c_ref, s_ref, *sems, n):
    side = Gather(n, _attention_weights((wq_ref, wk_ref, wv_ref, wo_ref), 0, wa_out), sems)
    side.start()
    some, width = 32, c_ref.shape[1]
    lane = lax.broadcasted_iota(jnp.int32, (some, width), 1)

    def tables(j, _):
        here = pl.ds(pl.multiple_of(j * some, some), some)
        angle = (lax.broadcasted_iota(jnp.int32, (some, width), 0) + j * some).astype(F32) * speed_ref[...]
        c_ref[here, :] = jnp.cos(angle)
        sin = jnp.sin(angle)
        s_ref[here, :] = jnp.where(lane < width // 2, -sin, sin)

    lax.fori_loop(0, c_ref.shape[0] // some, tables, None)
    lax.fori_loop(0, side.events, lambda k, _: side.event(k), None)
    side.finish()


def fetched(blocks, t, d, n, comm):
    half = HEAD // 2
    speed = THETA ** (-jnp.arange(half, dtype=F32) / half)
    table = jax.ShapeDtypeStruct((t, HEAD), F32)
    vmem = pl.BlockSpec(memory_space=pltpu.VMEM)
    return _call(functools.partial(_first_kernel, n=n), (), [ANY] * 4 + [vmem], [ANY, vmem, vmem],
                 [_out(d, sum(w.shape[2] for w in blocks)), table, table], Gather.scratch(n, 4), comm=comm)(*blocks, jnp.concatenate([speed, speed])[None])


def _ffn_back_kernel(by_ref, h_ref, o_ref, wgu_ref, wd_ref, wa_ref, *rest, bc, n, carries, unroll):
    if carries:
        mine_ref, dy_ref, do_ref, delta_ref, gw_ref, sum_ref, agu, ad, ao, db_s, down, *scratch = rest
        side = Scatter(n, mine_ref, sum_ref, CARRIED, scratch)
    else:
        dy_ref, do_ref, delta_ref, gw_ref, agu, ad, ao, db_s, down = rest
    i, last = pl.program_id(0), pl.num_programs(0) - 1
    f, d = wd_ref.shape
    g = do_ref.shape[0]
    bt = by_ref.shape[0]

    @pl.when(i == 0)
    def _():
        if carries:
            side.start()
        agu[...] = jnp.zeros_like(agu)
        ad[...] = jnp.zeros_like(ad)
        ao[...] = jnp.zeros_like(ao)

    by = by_ref[...]
    wide = h_ref[...].astype(F32)
    b = _normed(wide)
    bT, byT = b.T, by.T

    def chunk(j, _):
        here, there = pl.ds(pl.multiple_of(j * bc, bc), bc), pl.ds(pl.multiple_of(f + j * bc, bc), bc)
        gate = _dot(b, wgu_ref[:, here], 1, 0)
        up = _dot(b, wgu_ref[:, there], 1, 0)
        da = _dot(by, wd_ref[here, :], 1, 1).astype(BF16).astype(F32)
        sig = lax.logistic(gate)
        silu = gate * sig
        act = (silu * up).astype(BF16)
        dup = (da * silu).astype(BF16)
        dgate = (da * up * (sig + silu * (1 - sig))).astype(BF16)
        ad[:, here] += _dot(byT, act, 1, 0)
        agu[:, here] += _dot(bT, dgate, 1, 0)
        agu[:, there] += _dot(bT, dup, 1, 0)
        db_s[...] += _dot(dgate, wgu_ref[:, here], 1, 1) + _dot(dup, wgu_ref[:, there], 1, 1)

    db_s[...] = jnp.zeros_like(db_s)
    if unroll:
        for j in range(f // bc):
            chunk(j, None)
    else:
        lax.fori_loop(0, f // bc, chunk, None)
    db = db_s[...]
    dy = _norm_back(wide, db, by.astype(F32))
    dy_ref[...] = dy
    o = o_ref[...]
    do = _dot(dy, wa_ref[:, wa_ref.shape[1] - d :], 1, 1).astype(BF16)
    ao[...] += _dot(o.T, dy, 1, 0)
    prod = do.astype(F32) * o.astype(F32)
    lane = lax.broadcasted_iota(jnp.int32, (bt, HEAD), 1)
    deltas = jnp.zeros((bt, HEAD), F32)
    for m in range(g):
        do_ref[m] = do[:, m * HEAD : (m + 1) * HEAD]
        deltas = jnp.where(lane == m, prod[:, m * HEAD : (m + 1) * HEAD].sum(-1, keepdims=True), deltas)
    delta_ref[...] = deltas.T[:g, :]

    @pl.when(i == last)
    def _():
        r, rd, ro = d // n, f // n, ao.shape[0] // n
        down[...] = ad[...].astype(BF16).T

        def cut(owner, _):
            mine = gw_ref.at[lax.rem(owner, CORES), lax.div(owner, CORES)]
            rows = lambda size: pl.ds(pl.multiple_of(owner * size, size), size)
            top = 0
            for c in range(0, 2 * f, d):
                mine[top : top + r, :] = agu[rows(r), c : c + d].astype(BF16)
                top += r
            mine[top : top + rd, :] = down[rows(rd), :]
            mine[top + rd : top + rd + ro, :] = ao[rows(ro), :].astype(BF16)

        lax.fori_loop(0, n, cut, None)

    if carries:
        _events(side, i, range(BACK_STEPS), CARRIED, i == last)


BACK_STEPS = 4
CARRIED = 1


def ffn_back(by, h, o, wgu, wd, wa, n, mine=None, comm=None, bc=512, unroll=True):
    t, d = h.shape
    bt = t // BACK_STEPS
    f = wd.shape[0]
    carries = mine is not None
    rows = (2 * d * f + f * d + o.shape[1] * d) // n // d
    g = o.shape[1] // HEAD
    return _call(
        functools.partial(_ffn_back_kernel, bc=bc, n=n, carries=carries, unroll=unroll), (BACK_STEPS,),
        [_rows(bt, d), _rows(bt, d), _rows(bt, g * HEAD), _whole(*wgu.shape), _whole(*wd.shape), _whole(*wa.shape)] + [ANY] * carries,
        [_rows(bt, d), _heads(g, bt, HEAD), pl.BlockSpec((g, bt), lambda i: (0, i)), _whole(CORES, n // CORES, rows, d)]
        + ([_whole(*mine.shape[2:])] if carries else []),
        [_out(t, d), _out(g, t, HEAD), jax.ShapeDtypeStruct((g, t), F32), _out(CORES, n // CORES, rows, d)]
        + ([_out(*mine.shape[2:])] if carries else []),
        [pltpu.VMEM((d, 2 * f), F32), pltpu.VMEM((d, f), F32), pltpu.VMEM((g * HEAD, d), F32), pltpu.VMEM((bt, d), F32), pltpu.VMEM((f, d), BF16)]
        + (Scatter.scratch(n, *mine.shape[2:], CARRIED) if carries else []),
        flops=2 * t * d * (8 * f + 2 * g * HEAD), size=2 * (5 * t * d + 2 * wgu.size + 2 * wd.size + wa.size), exps=t * f, comm=comm,
    )(by, h, o, wgu, wd, wa, *([mine] if carries else []))


def _attend_back_kernel(q_ref, k_ref, v_ref, do_ref, lse_ref, delta_ref, h_ref, c_ref, s_ref, w_ref, mine_ref, *rest, wide, n, onward, marks, per):
    if onward:
        by_ref, dy_ref, *rest = rest
    gw_ref, sum_ref, dq_s, dk_s, dv_s, gap_s, acc, *scratch = rest
    g, bq, d = q_ref.shape
    bk, cols = bq, g * bq
    i, blocks = pl.program_id(0), k_ref.shape[0] // bq
    iq = blocks - 1 - i
    scale = d**-0.5
    e = scale * LOG2E
    at_all = range(0, cols, wide)
    side = Scatter(n, mine_ref, sum_ref, PIECES, scratch)

    @pl.when(i == 0)
    def _():
        side.start()
        gap_s[...] = _gap(bk, cols, bq)
        dk_s[...] = jnp.zeros_like(dk_s)
        dv_s[...] = jnp.zeros_like(dv_s)
        acc[...] = jnp.zeros_like(acc)

    dq_s[...] = jnp.zeros_like(dq_s)
    site = i * blocks - lax.div(i * (i - 1), 2)
    lse = jnp.concatenate([lse_ref[m : m + 1, :] for m in range(g)], axis=1) * LOG2E
    delta = jnp.concatenate([delta_ref[m : m + 1, :] for m in range(g)], axis=1)

    def block(j, masked):
        here = pl.ds(pl.multiple_of(j * bk, bk), bk)
        qs = [q_ref[...].reshape(cols, d)[at : at + wide, :] for at in at_all]
        dos = [do_ref[...].reshape(cols, d)[at : at + wide, :] for at in at_all]
        scores = [_dot(k_ref[here, :], x, 1, 1) for x in qs]
        dps = [_dot(v_ref[here, :], x, 1, 1) for x in dos]
        for m, at in enumerate(at_all):
            p = jnp.exp2(scores[m] * e - lse[:, at : at + wide])
            if masked:
                p = jnp.where(gap_s[:, at : at + wide] >= 0, p, 0.0)
            ds = (p * (dps[m] - delta[:, at : at + wide])).astype(BF16)
            dv_s[here, :] += _dot(p.astype(BF16), dos[m], 1, 0)
            dk_s[here, :] += _dot(ds, qs[m], 1, 0)
            dq_s[:, at : at + wide] += _dot(k_ref[here, :].T, ds, 1, 0)
        if not masked:
            _events(side, site + j, marks, per)

    lax.fori_loop(0, iq, lambda j, _: block(j, False), None)
    block(iq, True)
    here = pl.ds(pl.multiple_of(iq * bq, bq), bq)
    dq = (dq_s[...] * scale).astype(BF16).T
    c, s = c_ref[...], s_ref[...]
    parts = []
    for m in range(g + 1):
        t = (dq[m * bq : (m + 1) * bq, :] if m < g else (dk_s[here, :] * scale).astype(BF16)).astype(F32)
        parts.append((t * c - pltpu.roll(t, d // 2, 1) * s).astype(BF16))
    by_qkv = jnp.concatenate(parts + [dv_s[here, :].astype(BF16)], axis=1)
    x = h_ref[...].astype(F32)
    acc[...] += _dot(_normed(x).T, by_qkv, 1, 0)
    if onward:
        dy_ref[...] = _norm_back(x, _dot(by_qkv, w_ref[:, : by_qkv.shape[1]], 1, 1), by_ref[...].astype(F32))

    @pl.when(i == blocks - 1)
    def _():
        width, r = g * d, acc.shape[0] // n

        def cut(owner, _):
            block = gw_ref.at[lax.rem(owner, CORES), lax.div(owner, CORES)]
            at = pl.multiple_of(owner * r, r)
            block[:r, :] = acc[pl.ds(at, r), :width].astype(BF16)
            block[r:, : 2 * d] = acc[pl.ds(at, r // 2), width:].astype(BF16)
            block[r:, 2 * d :] = acc[pl.ds(at + r // 2, r // 2), width:].astype(BF16)

        lax.fori_loop(0, n, cut, None)

    _events(side, site + iq, marks, per, i == blocks - 1)


PIECES = 4


def attend_back(q, k, v, do, lse, delta, h, c, s, w, by, mine, n, comm, bq=512, wide=512, marks=range(1, 11), per=2):
    g, t, _ = q.shape
    d = h.shape[1]
    bq = min(bq, t)
    steps = t // bq
    onward = by is not None
    rows = lambda *rest: pl.BlockSpec((bq, *rest), lambda i: (steps - 1 - i,) + (0,) * len(rest))
    heads = pl.BlockSpec((g, bq, HEAD), lambda i: (0, steps - 1 - i, 0))
    stats = pl.BlockSpec((g, bq), lambda i: (0, steps - 1 - i))
    shape, cols = (CORES, n // CORES, 3 * d // n // 2, g * HEAD), (g + 2) * HEAD
    return _call(
        functools.partial(_attend_back_kernel, wide=wide, n=n, onward=onward, marks=marks, per=per), (steps,),
        [heads, _whole(t, HEAD), _whole(t, HEAD), heads, stats, stats, rows(d), rows(HEAD), rows(HEAD), _whole(*w.shape), ANY] + [rows(d)] * onward,
        [rows(d)] * onward + [_whole(*shape), _whole(*mine.shape[2:])],
        [_out(t, d)] * onward + [_out(*shape), _out(*mine.shape[2:])],
        [pltpu.VMEM((HEAD, g * bq), F32), pltpu.VMEM((t, HEAD), F32), pltpu.VMEM((t, HEAD), F32), pltpu.VMEM((bq, g * bq), jnp.int32),
         pltpu.VMEM((d, cols), F32), *Scatter.scratch(n, *mine.shape[2:], PIECES)],
        flops=5 * g * t * t * HEAD + 4 * t * d * cols, size=2 * t * HEAD * (3 * g + 4), exps=g * t * t // 2, comm=comm,
    )(q, k, v, do, lse, delta, h, c, s, w, mine, *([by] if onward else []))


def _last_kernel(mine_ref, *rest, n, given, pieces):
    refs, (sum_ref, all_ref, box, square_send, square_recv), scratch = rest[:given], rest[given : given + 5], rest[given + 5 :]
    side = Scatter(n, mine_ref, sum_ref, pieces, scratch)
    r = side.ring
    me = r.me
    barrier = pltpu.get_barrier_semaphore()
    away = lambda i: lax.rem(me + i, n)
    greet = lambda i, _: pl.semaphore_signal(barrier, inc=1, device_id={"dp": away(i)}, device_id_type=MESH)
    lax.fori_loop(1, n, greet, None)
    pl.semaphore_wait(barrier, n - 1)
    side.start(meet=False)
    square = lambda ref: jnp.sum(ref[...].astype(F32) ** 2)
    total = sum(square(ref) for ref in refs)
    lax.fori_loop(0, side.events, lambda k, _: side.event(k), None)
    box[me] = jnp.full(box.shape[1:], total + square(sum_ref), F32)
    post = lambda i: _send(box.at[me], box.at[me], square_send.at[i], square_recv.at[me], away(i))
    come = lambda i: _send(box.at[away(i)], box.at[away(i)], square_send.at[i], square_recv.at[away(i)], away(i))
    lax.fori_loop(1, n, lambda i, _: post(i).start(), None)
    lax.fori_loop(1, n, lambda i, _: come(i).wait_recv(), None)
    whole = box[0]
    for i in range(1, n):
        whole = whole + box[i]
    all_ref[...] = whole
    lax.fori_loop(1, n, lambda i, _: post(i).wait_send(), None)
    side.finish()


def last(mine, sums, n, comm, pieces=3):
    rows, cols = mine.shape[2:]
    tile = (8, 128)
    dma = pltpu.SemaphoreType.DMA
    vmem = pl.BlockSpec(memory_space=pltpu.VMEM)
    return _call(
        functools.partial(_last_kernel, n=n, given=len(sums), pieces=pieces), (), [ANY] + [vmem] * len(sums), [vmem, vmem],
        [_out(rows, cols), jax.ShapeDtypeStruct(tile, F32)],
        [pltpu.VMEM((n, *tile), F32), dma((n,)), dma((n,)), *Scatter.scratch(n, rows, cols, pieces)], comm=comm,
    )(mine, *sums)


def _adamw_kernel(*refs, layers, count):
    sums, (square,), refs = refs[: 2 * layers], refs[2 * layers : 2 * layers + 1], refs[2 * layers + 1 :]
    weights, ms, vs, new_w, new_m, new_v = (refs[i : i + 7] for i in range(0, 42, 7))
    factor = jnp.minimum(1.0, 0.5 * lax.rsqrt(square[:1, :1] / count + 1e-30))

    def take(which, layer, rows, cols, g):
        g = g.astype(F32) * factor
        at = (layer, rows, cols)
        m = 0.9 * ms[which][at] + 0.1 * g
        v = 0.95 * vs[which][at] + 0.05 * g * g
        w = weights[which][at].astype(F32)
        new_w[which][at] = (w - 0.02 * (m * lax.rsqrt(v + 1e-8) + 0.1 * w)).astype(BF16)
        new_m[which][at], new_v[which][at] = m, v

    whole = slice(None)
    for layer in range(layers):
        qkv, rest = sums[2 * layer], sums[2 * layer + 1]
        r, d = weights[0].shape[1], rest.shape[1]
        take(0, layer, whole, whole, qkv[:r, :])
        for half in range(2):
            rows = slice(half * (r // 2), (half + 1) * (r // 2))
            for which in range(2):
                at = (2 * half + which) * HEAD
                take(1 + which, layer, rows, whole, qkv[r:, at : at + HEAD])
        top = 0
        for which in (4, 5):
            for c in range(0, weights[which].shape[2], d):
                take(which, layer, whole, slice(c, c + d), rest[top : top + r, :])
                top += r
        for which in (6, 3):
            size = weights[which].shape[1]
            take(which, layer, whole, whole, rest[top : top + size, :])
            top += size


def adamw(sums, square, weights, m, v, n):
    layers = weights[0].shape[0]
    vmem = pl.BlockSpec(memory_space=pltpu.VMEM)
    count = n * sum(w.size for w in weights)
    return _call(
        functools.partial(_adamw_kernel, layers=layers, count=float(count)), (), [vmem] * (2 * layers + 22), [vmem] * 21,
        [jax.ShapeDtypeStruct(a.shape, a.dtype) for a in (*weights, *m, *v)],
    )(*sums, square, *weights, *m, *v)


def solution(mesh):
    def step(x, dy, *arrays):
        weights, m, v = (arrays[i : i + 7] for i in (0, 7, 14))
        wq, wk, wv, wo, wg, wu, wd = weights
        layers, n = wq.shape[0], mesh.shape["dp"]
        heads = wo.shape[1] * n // HEAD
        ids = iter(range(1, 100))
        h, kept = x[0], []
        wa, c, s = fetched((wq, wk, wv, wo), *h.shape, n, next(ids))
        for layer in range(layers):
            q, k, val, o, lse, h1, wgu, wdn = attend(h, wa, c, s, wg, wu, wd, heads, layer, n, next(ids))
            kept.append((h, q, k, val, o, lse, h1, wa, wgu, wdn))
            if layer < layers - 1:
                h, wa = ffn(h1, wgu, wdn, (wq, wk, wv, wo), layer + 1, n, next(ids))
        by, sums, mine = dy[0], [None] * (2 * layers), None
        for layer in reversed(range(layers)):
            h, q, k, val, o, lse, h1, wa, wgu, wdn = kept[layer]
            if mine is None:
                by, do, delta, rest = ffn_back(by, h1, o, wgu, wdn, wa, n)
            else:
                by, do, delta, rest, sums[2 * layer + 2] = ffn_back(by, h1, o, wgu, wdn, wa, n, mine, next(ids))
            *onward, mine, sums[2 * layer + 1] = attend_back(q, k, val, do, lse, delta, h, c, s, wa, by if layer else None, rest, n, next(ids))
            by = onward[0] if onward else None
        sums[0], square = last(mine, sums[1:], n, next(ids))
        return tuple(adamw(sums, square, weights, m, v, n))

    states, cut = P(("rep", "dp"), None, None), P(None, "dp", None)
    return jax.shard_map(
        step,
        mesh=mesh,
        in_specs=(states, states) + (cut,) * 21,
        out_specs=(P("rep", "dp", None),) * 21,
        check_vma=False,
    )
```

```python
import functools

import jax
import jax.numpy as jnp
from jax import lax
from jax.experimental import pallas as pl
from jax.experimental.pallas import tpu as pltpu
from jax.sharding import PartitionSpec as P

HEAD = 128
THETA = 10000
NEG = -1e30
HIDDEN = 2 * NEG
LOG2E = 1.4426950408889634
VMEM = 60 * 2**20
NAMES = ("wq", "wk", "wv", "wo", "w_gate", "w_up", "w_down")
F32, BF16 = jnp.float32, jnp.bfloat16


def _dot(a, b, ca, cb):
    return lax.dot_general(a, b, (((ca,), (cb,)), ((), ())), preferred_element_type=F32)


def _scale(wide):
    return lax.rsqrt(jnp.mean(wide * wide, -1, keepdims=True) + 1e-6)


def _normed(wide):
    return (wide * _scale(wide)).astype(BF16)


def _norm_back(wide, by, by_out):
    by = by.astype(BF16).astype(F32)
    s = _scale(wide)
    inner = s * by - wide * (s * s * s * jnp.mean(wide * by, -1, keepdims=True))
    return (by_out + inner.astype(BF16).astype(F32)).astype(BF16)


def _call(body, grid, ins, outs, shapes, scratch=(), flops=0, size=0, exps=0, comm=None):
    return pl.pallas_call(
        body,
        grid=grid,
        in_specs=ins,
        out_specs=outs,
        out_shape=shapes,
        scratch_shapes=list(scratch),
        compiler_params=pltpu.CompilerParams(dimension_semantics=("arbitrary",) * len(grid), vmem_limit_bytes=VMEM, collective_id=comm,
                                             has_side_effects=comm is not None),
        cost_estimate=pl.CostEstimate(flops=flops, bytes_accessed=size, transcendentals=exps),
    )


def _whole(*shape):
    return pl.BlockSpec(shape, lambda i: (0,) * len(shape), pipeline_mode=pl.Buffered(1))


def _rows(n, *rest):
    return pl.BlockSpec((n, *rest), lambda i: (i,) + (0,) * len(rest))


def _heads(h, n, *rest):
    return pl.BlockSpec((h, n, *rest), lambda i: (0, i) + (0,) * len(rest))


def _out(*shape):
    return jax.ShapeDtypeStruct(shape, BF16)


CORES = 2
MESH = pl.DeviceIdType.MESH
ANY = pl.BlockSpec(memory_space=pl.ANY)


class Ring:
    def __init__(self, n):
        self.n, self.chips = n, n // CORES
        self.long = self.chips // 2
        self.short = self.chips - 1 - self.long
        me = lax.axis_index("dp")
        self.me, self.z, self.core = me, lax.div(me, CORES), lax.rem(me, CORES)
        self.other = self.at(self.z, 1 - self.core)

    def chip(self, away):
        return lax.rem(self.z + away + self.chips, self.chips)

    def at(self, z, core):
        return z * CORES + core

    def to(self, away):
        return self.at(self.chip(away), self.core)

    def meet(self, reach=1):
        barrier = pltpu.get_barrier_semaphore()
        for device in (self.other, *(self.to(sign * i) for i in range(1, reach + 1) for sign in (1, -1))):
            pl.semaphore_signal(barrier, inc=1, device_id={"dp": device}, device_id_type=MESH)
        pl.semaphore_wait(barrier, 1 + 2 * reach)


def _send(src, dst, send, recv, device):
    return pltpu.make_async_remote_copy(src_ref=src, dst_ref=dst, send_sem=send, recv_sem=recv, device_id={"dp": device}, device_id_type=MESH)


class Gather:
    @staticmethod
    def scratch(n, count):
        dma, chips = pltpu.SemaphoreType.DMA, n // CORES
        return [dma((count, chips - 1)), dma((count, chips - 1)), dma((count, chips)), dma((count, chips)), dma((count,))]

    def __init__(self, n, groups, sems, reach=1):
        self.ring, self.groups, self.reach = Ring(n), groups, reach
        self.ring_send, self.ring_recv, self.pair_send, self.pair_recv, self.own = sems
        self.events = len(groups) * self.ring.long
        self.index = {}
        for number, group in enumerate(groups):
            for entry in range(len(group)):
                self.index[number, entry] = len(self.index)

    def place(self, item, owner):
        block, whole, column = item
        rows, cols = block.shape
        return whole.at[pl.ds(pl.multiple_of(owner * rows, rows), rows), pl.ds(column, cols)]

    def hop(self, x, item, slot, owner, device, first=False):
        place = self.place(item, owner)
        return _send(item[0] if first else place, place, self.ring_send.at[x, slot], self.ring_recv.at[x, slot], device)

    def pair(self, x, item, slot, owner, first=False):
        place = self.place(item, owner)
        return _send(item[0] if first else place, place, self.pair_send.at[x, slot], self.pair_recv.at[x, slot], self.ring.other)

    def each(self):
        for number, group in enumerate(self.groups):
            for entry, item in enumerate(group):
                yield self.index[number, entry], item, 1 - 2 * (number % 2)

    def start(self):
        r = self.ring
        r.meet(self.reach)
        for x, item, way in self.each():
            for i in range(self.reach):
                self.hop(x, item, i, r.me, r.to(way * (i + 1)), True).start()
                self.hop(x, item, r.long + i, r.me, r.to(-way * (i + 1)), True).start()
            self.pair(x, item, 0, r.me, True).start()
            pltpu.make_async_copy(item[0], self.place(item, r.me), self.own.at[x]).start()

    def event(self, k):
        r = self.ring
        t = lax.div(k, len(self.groups)) + 1
        for number, group in enumerate(self.groups):

            @pl.when(lax.rem(k, len(self.groups)) == number)
            def _():
                way = 1 - 2 * (number % 2)
                for entry, item in enumerate(group):
                    x = self.index[number, entry]
                    owner = r.to(-way * t)
                    self.hop(x, item, t - 1, owner, r.to(way)).wait_recv()

                    for i in range(self.reach):

                        @pl.when((lax.rem(t, self.reach) == 0) & (t + i < r.long))
                        def _():
                            self.hop(x, item, t + i, owner, r.to(way * (i + 1))).start()

                    self.pair(x, item, t, owner).start()

                    @pl.when(t <= r.short)
                    def _():
                        owner = r.to(way * t)
                        self.hop(x, item, r.long + t - 1, owner, r.to(-way)).wait_recv()

                        for i in range(self.reach):

                            @pl.when((lax.rem(t, self.reach) == 0) & (t + i < r.short))
                            def _():
                                self.hop(x, item, r.long + t + i, owner, r.to(-way * (i + 1))).start()

                        self.pair(x, item, r.long + t, owner).start()

    def finish(self):
        r = self.ring
        for x, item, way in self.each():
            pltpu.make_async_copy(item[0], self.place(item, r.me), self.own.at[x]).wait()

            def hop(slot, _):
                self.hop(x, item, slot, r.me, r.to(1)).wait_send()

            def pair(slot, _):
                away = jnp.where(slot <= r.long, -way * slot, way * (slot - r.long))
                self.pair(x, item, slot, r.me).wait_send()
                self.pair(x, item, slot, r.at(r.chip(away), 1 - r.core)).wait_recv()

            lax.fori_loop(0, r.chips - 1, hop, None)
            lax.fori_loop(0, r.chips, pair, None)


class Scatter:
    @staticmethod
    def scratch(n, rows, cols, pieces):
        dma, chips = pltpu.SemaphoreType.DMA, n // CORES
        return [pltpu.VMEM((chips, rows, cols), BF16), pltpu.VMEM((chips, rows, cols), BF16), pltpu.VMEM((chips - 1, rows, cols), BF16),
                dma((pieces,)), dma((pieces,)), dma((pieces,)), dma((pieces, chips - 1)), dma((pieces, chips - 1))]

    def __init__(self, n, mine, out, pieces, scratch):
        self.ring, self.mine, self.out, self.pieces = Ring(n), mine, out, pieces
        self.own, self.sum, self.got, self.own_sem, self.pair_send, self.pair_recv, self.ring_send, self.ring_recv = scratch
        self.events = pieces * (self.ring.long + 1)
        self.size = out.shape[0] // pieces

    def rows(self, a):
        return pl.ds(pl.multiple_of(a * self.size, self.size), self.size)

    def pair(self, a):
        return _send(self.mine.at[1 - self.ring.core, :, self.rows(a), :], self.sum.at[:, self.rows(a), :], self.pair_send.at[a], self.pair_recv.at[a],
                     self.ring.other)

    def own_copy(self, a):
        return pltpu.make_async_copy(self.mine.at[self.ring.core, :, self.rows(a), :], self.own.at[:, self.rows(a), :], self.own_sem.at[a])

    def hop(self, a, slot, chip, device):
        return _send(self.sum.at[chip, self.rows(a), :], self.got.at[slot, self.rows(a), :], self.ring_send.at[a, slot], self.ring_recv.at[a, slot], device)

    def start(self, meet=True):
        if meet:
            self.ring.meet()
        for a in range(self.pieces):
            self.pair(a).start()
            self.own_copy(a).start()

    def here(self, a, chip):
        return self.own[chip, self.rows(a), :].astype(F32) + self.sum[chip, self.rows(a), :].astype(F32)

    def add(self, a, slot):
        return self.got[slot, self.rows(a), :].astype(F32)

    def put(self, a, slot, chip, device, value):
        self.sum[chip, self.rows(a), :] = value.astype(BF16)
        self.hop(a, slot, chip, device).start()

    def event(self, k):
        r = self.ring
        t, a = lax.div(k, self.pieces), lax.rem(k, self.pieces)
        way = 1 - 2 * lax.rem(a, 2)
        far, near = r.chip(way * (r.long - t)), r.chip(-way * (r.short - t))

        @pl.when(t == 0)
        def _():
            self.own_copy(a).wait()
            self.pair(a).wait_recv()
            self.put(a, 0, far, r.to(way), self.here(a, far))
            self.put(a, r.long, near, r.to(-way), self.here(a, near))

        @pl.when((t > 0) & (t < r.long))
        def _():
            self.hop(a, t - 1, far, r.to(way)).wait_recv()
            self.put(a, t, far, r.to(way), self.here(a, far) + self.add(a, t - 1))

        @pl.when((t > 0) & (t < r.short))
        def _():
            self.hop(a, r.long + t - 1, near, r.to(-way)).wait_recv()
            self.put(a, r.long + t, near, r.to(-way), self.here(a, near) + self.add(a, r.long + t - 1))

        @pl.when(t == r.long)
        def _():
            one, two = r.long - 1, r.chips - 2
            self.hop(a, one, r.z, r.to(way)).wait_recv()
            self.hop(a, two, r.z, r.to(-way)).wait_recv()
            self.out[self.rows(a), :] = (self.here(a, r.z) + (self.add(a, one) + self.add(a, two))).astype(BF16)

    def finish(self):
        r = self.ring
        for a in range(self.pieces):
            self.pair(a).wait_send()
            lax.fori_loop(0, r.chips - 1, lambda slot, _: self.hop(a, slot, r.z, r.to(1)).wait_send(), None)


def _events(side, site, marks, per, last=None):
    upto = lambda at: jnp.minimum(per * sum((at > mark).astype(jnp.int32) for mark in marks), side.events)
    end = upto(site + 1) if last is None else jnp.where(last, side.events, upto(site + 1))
    lax.fori_loop(upto(site), end, lambda k, _: side.event(k), None)
    if last is not None:
        pl.when(last)(side.finish)


def _gap(bk, cols, bq):
    return lax.rem(lax.broadcasted_iota(jnp.int32, (bk, cols), 1), bq) - lax.broadcasted_iota(jnp.int32, (bk, cols), 0)


def _attend_kernel(h_ref, w_ref, c_ref, s_ref, wg_ref, wu_ref, wd_ref, q_ref, k_ref, v_ref, o_ref, lse_ref, y_ref, wgu_out, wd_out,
                   keys, values, top_s, mix_s, gap_s, *sems, wide, n, layer, marks):
    g, bq, d = q_ref.shape
    bk, cols = bq, g * bq
    iq, blocks = pl.program_id(0), keys.shape[0] // bq
    scale = d**-0.5
    e = scale * LOG2E
    at_all = range(0, cols, wide)
    f = wg_ref.shape[2]
    side = Gather(n, [[(wg_ref.at[layer], wgu_out, 0)], [(wu_ref.at[layer], wgu_out, f)], [(wd_ref.at[layer], wd_out, 0)]], sems)

    @pl.when(iq == 0)
    def _():
        side.start()
        gap_s[...] = _gap(bk, cols, bq)
        values[d:, :] = jnp.ones((8, values.shape[1]), BF16)

    mine = pl.ds(pl.multiple_of(iq * bq, bq), bq)
    r = _dot(_normed(h_ref[...].astype(F32)), w_ref[:, : (g + 2) * d], 1, 0).astype(BF16)
    c, s = c_ref[...], s_ref[...]
    for m in range(g + 1):
        t = r[:, m * d : (m + 1) * d].astype(F32)
        t = (t * c + pltpu.roll(t, d // 2, 1) * s).astype(BF16)
        if m < g:
            q_ref[m] = t
        else:
            k_ref[...] = t
            keys[mine, :] = t
    v = r[:, (g + 1) * d :]
    v_ref[...] = v
    values[:d, mine] = v.T
    top_s[...] = jnp.full_like(top_s, NEG)
    mix_s[...] = jnp.zeros_like(mix_s)

    site = lax.div(iq * (iq + 1), 2)

    def block(j, masked):
        here = pl.ds(pl.multiple_of(j * bk, bk), bk)
        qs = q_ref[...].reshape(cols, d)
        scores = [_dot(keys[here, :], qs[at : at + wide, :], 1, 1) for at in at_all]
        weights, keeps = [], []
        for at, s in zip(at_all, scores):
            if masked:
                s = jnp.where(gap_s[:, at : at + wide] >= 0, s, HIDDEN)
            old = top_s[:, at : at + wide]
            top = jnp.maximum(old, s.max(axis=0, keepdims=True))
            top_s[:, at : at + wide] = top
            weights.append(jnp.exp2((s - top) * e).astype(BF16))
            keeps.append(jnp.exp2((old - top) * e))
        for at, p, keep in zip(at_all, weights, keeps):
            mix_s[:, at : at + wide] = mix_s[:, at : at + wide] * keep + _dot(values[:, here], p, 1, 0)
        if not masked:
            _events(side, site + j, marks, 1)

    lax.fori_loop(0, iq, lambda j, _: block(j, False), None)
    block(iq, True)
    total = mix_s[d : d + 1, :]
    o = (mix_s[:d, :] * (1 / total)).astype(BF16)
    lse = top_s[...] * scale + jnp.log(total)
    for m in range(g):
        o_ref[:, m * d : (m + 1) * d] = o[:, m * bq : (m + 1) * bq].T
        lse_ref[m : m + 1, :] = lse[:, m * bq : (m + 1) * bq]
    out = _dot(o_ref[...], w_ref[:, w_ref.shape[1] - h_ref.shape[1] :], 1, 0).astype(BF16)
    y_ref[...] = (h_ref[...].astype(F32) + out.astype(F32)).astype(BF16)
    _events(side, site + iq, marks, 1, iq == blocks - 1)


def attend(h, w, c, s, wg, wu, wd, heads, layer, n, comm, bq=512, wide=512, marks=range(1, 10)):
    t, d = h.shape
    bq, g, f = min(bq, t), heads, wg.shape[2]
    return _call(
        functools.partial(_attend_kernel, wide=wide, n=n, layer=layer, marks=marks), (t // bq,),
        [_rows(bq, d), _whole(*w.shape), _rows(bq, HEAD), _rows(bq, HEAD), ANY, ANY, ANY],
        [_heads(g, bq, HEAD), _rows(bq, HEAD), _rows(bq, HEAD), _rows(bq, g * HEAD), pl.BlockSpec((g, bq), lambda i: (0, i)), _rows(bq, d), ANY, ANY],
        [_out(g, t, HEAD), _out(t, HEAD), _out(t, HEAD), _out(t, g * HEAD), jax.ShapeDtypeStruct((g, t), F32), _out(t, d), _out(d, 2 * f), _out(f, d)],
        [pltpu.VMEM((t, HEAD), BF16), pltpu.VMEM((HEAD + 8, t), BF16), pltpu.VMEM((1, g * bq), F32), pltpu.VMEM((HEAD + 8, g * bq), F32),
         pltpu.VMEM((bq, g * bq), jnp.int32), *Gather.scratch(n, 3)],
        flops=2 * g * t * t * HEAD + 2 * t * w.size, size=2 * t * (3 * g * HEAD + 2 * d), exps=g * t * t // 2, comm=comm,
    )(h, w, c, s, wg, wu, wd)


def _attention_weights(refs, layer, whole):
    group, column = [], 0
    for ref in refs:
        group.append((ref.at[layer], whole, column))
        column += ref.shape[2]
    return [group]


def _ffn_kernel(h_ref, wgu_ref, wd_ref, y_ref, *, bc):
    f = wd_ref.shape[0]
    wide = h_ref[...].astype(F32)
    b = _normed(wide)
    out = jnp.zeros(wide.shape, F32)
    for c in range(0, f, bc):
        gate = _dot(b, wgu_ref[:, c : c + bc], 1, 0)
        up = _dot(b, wgu_ref[:, f + c : f + c + bc], 1, 0)
        act = (gate * lax.logistic(gate) * up).astype(BF16)
        out += _dot(act, wd_ref[c : c + bc, :], 1, 0)
    y_ref[...] = (wide + out.astype(BF16).astype(F32)).astype(BF16)


def ffn(h, wgu, wd, bt=512, bc=512):
    t, d = h.shape
    bt = min(bt, t)
    return _call(
        functools.partial(_ffn_kernel, bc=bc), (t // bt,), [_rows(bt, d), _whole(*wgu.shape), _whole(*wd.shape)], _rows(bt, d), _out(t, d),
        flops=2 * t * (wgu.size + wd.size), size=2 * (2 * t * d + wgu.size + wd.size), exps=t * wd.shape[0],
    )(h, wgu, wd)


def _first_kernel(wq_ref, wk_ref, wv_ref, wo_ref, speed_ref, *rest, n, layers):
    wholes, (c_ref, s_ref), sems = rest[:layers], rest[layers : layers + 2], rest[layers + 2 :]
    refs = (wq_ref, wk_ref, wv_ref, wo_ref)
    side = Gather(n, [group for layer in range(layers) for group in _attention_weights(refs, layer, wholes[layer])], sems)
    side.start()
    some, width = 64, c_ref.shape[1]
    count = c_ref.shape[0] // some
    marks = range(count // 4, count, max(count // 10, 1))
    lane = lax.broadcasted_iota(jnp.int32, (some, width), 1)

    def tables(j, _):
        here = pl.ds(pl.multiple_of(j * some, some), some)
        angle = (lax.broadcasted_iota(jnp.int32, (some, width), 0) + j * some).astype(F32) * speed_ref[...]
        c_ref[here, :] = jnp.cos(angle)
        sin = jnp.sin(angle)
        s_ref[here, :] = jnp.where(lane < width // 2, -sin, sin)
        _events(side, j, marks, 1)

    lax.fori_loop(0, count, tables, None)
    lax.fori_loop(min(len(marks), side.events), side.events, lambda k, _: side.event(k), None)
    side.finish()


def fetched(blocks, t, d, n, comm):
    half = HEAD // 2
    speed = THETA ** (-jnp.arange(half, dtype=F32) / half)
    table = jax.ShapeDtypeStruct((t, HEAD), F32)
    vmem = pl.BlockSpec(memory_space=pltpu.VMEM)
    layers, whole = blocks[0].shape[0], _out(d, sum(w.shape[2] for w in blocks))
    return _call(functools.partial(_first_kernel, n=n, layers=layers), (), [ANY] * 4 + [vmem], [ANY] * layers + [vmem, vmem],
                 [whole] * layers + [table, table], Gather.scratch(n, 4 * layers), comm=comm)(*blocks, jnp.concatenate([speed, speed])[None])


def _ffn_back_kernel(by_ref, h_ref, o_ref, wgu_ref, wd_ref, wa_ref, *rest, bc, n, carries, unroll):
    if carries:
        mine_ref, dy_ref, do_ref, delta_ref, gw_ref, sum_ref, agu, ad, ao, db_s, down, *scratch = rest
        side = Scatter(n, mine_ref, sum_ref, CARRIED, scratch)
    else:
        dy_ref, do_ref, delta_ref, gw_ref, agu, ad, ao, db_s, down = rest
    i, last = pl.program_id(0), pl.num_programs(0) - 1
    f, d = wd_ref.shape
    g = do_ref.shape[0]
    bt = by_ref.shape[0]

    @pl.when(i == 0)
    def _():
        if carries:
            side.start()
        agu[...] = jnp.zeros_like(agu)
        ad[...] = jnp.zeros_like(ad)
        ao[...] = jnp.zeros_like(ao)

    by = by_ref[...]
    wide = h_ref[...].astype(F32)
    b = _normed(wide)
    bT, byT = b.T, by.T

    def chunk(j, _):
        here, there = pl.ds(pl.multiple_of(j * bc, bc), bc), pl.ds(pl.multiple_of(f + j * bc, bc), bc)
        gate = _dot(b, wgu_ref[:, here], 1, 0)
        up = _dot(b, wgu_ref[:, there], 1, 0)
        da = _dot(by, wd_ref[here, :], 1, 1).astype(BF16).astype(F32)
        sig = lax.logistic(gate)
        silu = gate * sig
        act = (silu * up).astype(BF16)
        dup = (da * silu).astype(BF16)
        dgate = (da * up * (sig + silu * (1 - sig))).astype(BF16)
        ad[:, here] += _dot(byT, act, 1, 0)
        agu[:, here] += _dot(bT, dgate, 1, 0)
        agu[:, there] += _dot(bT, dup, 1, 0)
        db_s[...] += _dot(dgate, wgu_ref[:, here], 1, 1) + _dot(dup, wgu_ref[:, there], 1, 1)

    db_s[...] = jnp.zeros_like(db_s)
    if unroll:
        for j in range(f // bc):
            chunk(j, None)
    else:
        lax.fori_loop(0, f // bc, chunk, None)
    db = db_s[...]
    dy = _norm_back(wide, db, by.astype(F32))
    dy_ref[...] = dy
    o = o_ref[...]
    do = _dot(dy, wa_ref[:, wa_ref.shape[1] - d :], 1, 1).astype(BF16)
    ao[...] += _dot(o.T, dy, 1, 0)
    prod = do.astype(F32) * o.astype(F32)
    lane = lax.broadcasted_iota(jnp.int32, (bt, HEAD), 1)
    deltas = jnp.zeros((bt, HEAD), F32)
    for m in range(g):
        do_ref[m] = do[:, m * HEAD : (m + 1) * HEAD]
        deltas = jnp.where(lane == m, prod[:, m * HEAD : (m + 1) * HEAD].sum(-1, keepdims=True), deltas)
    delta_ref[...] = deltas.T[:g, :]

    @pl.when(i == last)
    def _():
        r, rd, ro = d // n, f // n, ao.shape[0] // n
        down[...] = ad[...].astype(BF16).T

        def cut(owner, _):
            mine = gw_ref.at[lax.rem(owner, CORES), lax.div(owner, CORES)]
            rows = lambda size: pl.ds(pl.multiple_of(owner * size, size), size)
            top = 0
            for c in range(0, 2 * f, d):
                mine[top : top + r, :] = agu[rows(r), c : c + d].astype(BF16)
                top += r
            mine[top : top + rd, :] = down[rows(rd), :]
            mine[top + rd : top + rd + ro, :] = ao[rows(ro), :].astype(BF16)

        lax.fori_loop(0, n, cut, None)

    if carries:
        _events(side, i, range(BACK_STEPS), CARRIED, i == last)


BACK_STEPS = 4
CARRIED = 1


def ffn_back(by, h, o, wgu, wd, wa, n, mine=None, comm=None, bc=512, unroll=True):
    t, d = h.shape
    bt = t // BACK_STEPS
    f = wd.shape[0]
    carries = mine is not None
    rows = (2 * d * f + f * d + o.shape[1] * d) // n // d
    g = o.shape[1] // HEAD
    return _call(
        functools.partial(_ffn_back_kernel, bc=bc, n=n, carries=carries, unroll=unroll), (BACK_STEPS,),
        [_rows(bt, d), _rows(bt, d), _rows(bt, g * HEAD), _whole(*wgu.shape), _whole(*wd.shape), _whole(*wa.shape)] + [ANY] * carries,
        [_rows(bt, d), _heads(g, bt, HEAD), pl.BlockSpec((g, bt), lambda i: (0, i)), _whole(CORES, n // CORES, rows, d)]
        + ([_whole(*mine.shape[2:])] if carries else []),
        [_out(t, d), _out(g, t, HEAD), jax.ShapeDtypeStruct((g, t), F32), _out(CORES, n // CORES, rows, d)]
        + ([_out(*mine.shape[2:])] if carries else []),
        [pltpu.VMEM((d, 2 * f), F32), pltpu.VMEM((d, f), F32), pltpu.VMEM((g * HEAD, d), F32), pltpu.VMEM((bt, d), F32), pltpu.VMEM((f, d), BF16)]
        + (Scatter.scratch(n, *mine.shape[2:], CARRIED) if carries else []),
        flops=2 * t * d * (8 * f + 2 * g * HEAD), size=2 * (5 * t * d + 2 * wgu.size + 2 * wd.size + wa.size), exps=t * f, comm=comm,
    )(by, h, o, wgu, wd, wa, *([mine] if carries else []))


def _attend_back_kernel(q_ref, k_ref, v_ref, do_ref, lse_ref, delta_ref, h_ref, c_ref, s_ref, w_ref, mine_ref, *rest, wide, n, onward, marks, per):
    if onward:
        by_ref, dy_ref, *rest = rest
    gw_ref, sum_ref, dq_s, dk_s, dv_s, gap_s, acc, *scratch = rest
    g, bq, d = q_ref.shape
    bk, cols = bq, g * bq
    i, blocks = pl.program_id(0), k_ref.shape[0] // bq
    iq = blocks - 1 - i
    scale = d**-0.5
    e = scale * LOG2E
    at_all = range(0, cols, wide)
    side = Scatter(n, mine_ref, sum_ref, PIECES, scratch)

    @pl.when(i == 0)
    def _():
        side.start()
        gap_s[...] = _gap(bk, cols, bq)
        dk_s[...] = jnp.zeros_like(dk_s)
        dv_s[...] = jnp.zeros_like(dv_s)
        acc[...] = jnp.zeros_like(acc)

    dq_s[...] = jnp.zeros_like(dq_s)
    site = i * blocks - lax.div(i * (i - 1), 2)
    lse = jnp.concatenate([lse_ref[m : m + 1, :] for m in range(g)], axis=1) * LOG2E
    delta = jnp.concatenate([delta_ref[m : m + 1, :] for m in range(g)], axis=1)

    def block(j, masked):
        here = pl.ds(pl.multiple_of(j * bk, bk), bk)
        qs = [q_ref[...].reshape(cols, d)[at : at + wide, :] for at in at_all]
        dos = [do_ref[...].reshape(cols, d)[at : at + wide, :] for at in at_all]
        scores = [_dot(k_ref[here, :], x, 1, 1) for x in qs]
        dps = [_dot(v_ref[here, :], x, 1, 1) for x in dos]
        for m, at in enumerate(at_all):
            p = jnp.exp2(scores[m] * e - lse[:, at : at + wide])
            if masked:
                p = jnp.where(gap_s[:, at : at + wide] >= 0, p, 0.0)
            ds = (p * (dps[m] - delta[:, at : at + wide])).astype(BF16)
            dv_s[here, :] += _dot(p.astype(BF16), dos[m], 1, 0)
            dk_s[here, :] += _dot(ds, qs[m], 1, 0)
            dq_s[:, at : at + wide] += _dot(k_ref[here, :].T, ds, 1, 0)
        if not masked:
            _events(side, site + j, marks, per)

    lax.fori_loop(0, iq, lambda j, _: block(j, False), None)
    block(iq, True)
    here = pl.ds(pl.multiple_of(iq * bq, bq), bq)
    dq = (dq_s[...] * scale).astype(BF16).T
    c, s = c_ref[...], s_ref[...]
    parts = []
    for m in range(g + 1):
        t = (dq[m * bq : (m + 1) * bq, :] if m < g else (dk_s[here, :] * scale).astype(BF16)).astype(F32)
        parts.append((t * c - pltpu.roll(t, d // 2, 1) * s).astype(BF16))
    by_qkv = jnp.concatenate(parts + [dv_s[here, :].astype(BF16)], axis=1)
    x = h_ref[...].astype(F32)
    acc[...] += _dot(_normed(x).T, by_qkv, 1, 0)
    if onward:
        dy_ref[...] = _norm_back(x, _dot(by_qkv, w_ref[:, : by_qkv.shape[1]], 1, 1), by_ref[...].astype(F32))

    @pl.when(i == blocks - 1)
    def _():
        width, r = g * d, acc.shape[0] // n

        def cut(owner, _):
            block = gw_ref.at[lax.rem(owner, CORES), lax.div(owner, CORES)]
            at = pl.multiple_of(owner * r, r)
            block[:r, :] = acc[pl.ds(at, r), :width].astype(BF16)
            block[r:, : 2 * d] = acc[pl.ds(at, r // 2), width:].astype(BF16)
            block[r:, 2 * d :] = acc[pl.ds(at + r // 2, r // 2), width:].astype(BF16)

        lax.fori_loop(0, n, cut, None)

    _events(side, site + iq, marks, per, i == blocks - 1)


PIECES = 4


def attend_back(q, k, v, do, lse, delta, h, c, s, w, by, mine, n, comm, bq=512, wide=512, marks=range(1, 11), per=2):
    g, t, _ = q.shape
    d = h.shape[1]
    bq = min(bq, t)
    steps = t // bq
    onward = by is not None
    rows = lambda *rest: pl.BlockSpec((bq, *rest), lambda i: (steps - 1 - i,) + (0,) * len(rest))
    heads = pl.BlockSpec((g, bq, HEAD), lambda i: (0, steps - 1 - i, 0))
    stats = pl.BlockSpec((g, bq), lambda i: (0, steps - 1 - i))
    shape, cols = (CORES, n // CORES, 3 * d // n // 2, g * HEAD), (g + 2) * HEAD
    return _call(
        functools.partial(_attend_back_kernel, wide=wide, n=n, onward=onward, marks=marks, per=per), (steps,),
        [heads, _whole(t, HEAD), _whole(t, HEAD), heads, stats, stats, rows(d), rows(HEAD), rows(HEAD), _whole(*w.shape), ANY] + [rows(d)] * onward,
        [rows(d)] * onward + [_whole(*shape), _whole(*mine.shape[2:])],
        [_out(t, d)] * onward + [_out(*shape), _out(*mine.shape[2:])],
        [pltpu.VMEM((HEAD, g * bq), F32), pltpu.VMEM((t, HEAD), F32), pltpu.VMEM((t, HEAD), F32), pltpu.VMEM((bq, g * bq), jnp.int32),
         pltpu.VMEM((d, cols), F32), *Scatter.scratch(n, *mine.shape[2:], PIECES)],
        flops=5 * g * t * t * HEAD + 4 * t * d * cols, size=2 * t * HEAD * (3 * g + 4), exps=g * t * t // 2, comm=comm,
    )(q, k, v, do, lse, delta, h, c, s, w, mine, *([by] if onward else []))


def _last_kernel(mine_ref, *rest, n, given, pieces):
    refs, (sum_ref, all_ref, box, square_send, square_recv), scratch = rest[:given], rest[given : given + 5], rest[given + 5 :]
    side = Scatter(n, mine_ref, sum_ref, pieces, scratch)
    r = side.ring
    me = r.me
    barrier = pltpu.get_barrier_semaphore()
    away = lambda i: lax.rem(me + i, n)
    greet = lambda i, _: pl.semaphore_signal(barrier, inc=1, device_id={"dp": away(i)}, device_id_type=MESH)
    lax.fori_loop(1, n, greet, None)
    pl.semaphore_wait(barrier, n - 1)
    side.start(meet=False)
    square = lambda ref: jnp.sum(ref[...].astype(F32) ** 2)
    total = sum(square(ref) for ref in refs)
    lax.fori_loop(0, side.events, lambda k, _: side.event(k), None)
    box[me] = jnp.full(box.shape[1:], total + square(sum_ref), F32)
    post = lambda i: _send(box.at[me], box.at[me], square_send.at[i], square_recv.at[me], away(i))
    come = lambda i: _send(box.at[away(i)], box.at[away(i)], square_send.at[i], square_recv.at[away(i)], away(i))
    lax.fori_loop(1, n, lambda i, _: post(i).start(), None)
    lax.fori_loop(1, n, lambda i, _: come(i).wait_recv(), None)
    whole = box[0]
    for i in range(1, n):
        whole = whole + box[i]
    all_ref[...] = whole
    lax.fori_loop(1, n, lambda i, _: post(i).wait_send(), None)
    side.finish()


def last(mine, sums, n, comm, pieces=3):
    rows, cols = mine.shape[2:]
    tile = (8, 128)
    dma = pltpu.SemaphoreType.DMA
    vmem = pl.BlockSpec(memory_space=pltpu.VMEM)
    return _call(
        functools.partial(_last_kernel, n=n, given=len(sums), pieces=pieces), (), [ANY] + [vmem] * len(sums), [vmem, vmem],
        [_out(rows, cols), jax.ShapeDtypeStruct(tile, F32)],
        [pltpu.VMEM((n, *tile), F32), dma((n,)), dma((n,)), *Scatter.scratch(n, rows, cols, pieces)], comm=comm,
    )(mine, *sums)


def _adamw_kernel(*refs, layers, count):
    sums, (square,), refs = refs[: 2 * layers], refs[2 * layers : 2 * layers + 1], refs[2 * layers + 1 :]
    weights, ms, vs, new_w, new_m, new_v = (refs[i : i + 7] for i in range(0, 42, 7))
    factor = jnp.minimum(1.0, 0.5 * lax.rsqrt(square[:1, :1] / count + 1e-30))

    def take(which, layer, rows, cols, g):
        g = g.astype(F32) * factor
        at = (layer, rows, cols)
        m = 0.9 * ms[which][at] + 0.1 * g
        v = 0.95 * vs[which][at] + 0.05 * g * g
        w = weights[which][at].astype(F32)
        new_w[which][at] = (w - 0.02 * (m * lax.rsqrt(v + 1e-8) + 0.1 * w)).astype(BF16)
        new_m[which][at], new_v[which][at] = m, v

    whole = slice(None)
    for layer in range(layers):
        qkv, rest = sums[2 * layer], sums[2 * layer + 1]
        r, d = weights[0].shape[1], rest.shape[1]
        take(0, layer, whole, whole, qkv[:r, :])
        for half in range(2):
            rows = slice(half * (r // 2), (half + 1) * (r // 2))
            for which in range(2):
                at = (2 * half + which) * HEAD
                take(1 + which, layer, rows, whole, qkv[r:, at : at + HEAD])
        top = 0
        for which in (4, 5):
            for c in range(0, weights[which].shape[2], d):
                take(which, layer, whole, slice(c, c + d), rest[top : top + r, :])
                top += r
        for which in (6, 3):
            size = weights[which].shape[1]
            take(which, layer, whole, whole, rest[top : top + size, :])
            top += size


def adamw(sums, square, weights, m, v, n):
    layers = weights[0].shape[0]
    vmem = pl.BlockSpec(memory_space=pltpu.VMEM)
    count = n * sum(w.size for w in weights)
    return _call(
        functools.partial(_adamw_kernel, layers=layers, count=float(count)), (), [vmem] * (2 * layers + 22), [vmem] * 21,
        [jax.ShapeDtypeStruct(a.shape, a.dtype) for a in (*weights, *m, *v)],
    )(*sums, square, *weights, *m, *v)


def solution(mesh):
    def step(x, dy, *arrays):
        weights, m, v = (arrays[i : i + 7] for i in (0, 7, 14))
        wq, wk, wv, wo, wg, wu, wd = weights
        layers, n = wq.shape[0], mesh.shape["dp"]
        heads = wo.shape[1] * n // HEAD
        ids = iter(range(1, 100))
        h, kept = x[0], []
        *attention, c, s = fetched((wq, wk, wv, wo), *h.shape, n, next(ids))
        for layer, wa in enumerate(attention):
            q, k, val, o, lse, h1, wgu, wdn = attend(h, wa, c, s, wg, wu, wd, heads, layer, n, next(ids))
            kept.append((h, q, k, val, o, lse, h1, wa, wgu, wdn))
            if layer < layers - 1:
                h = ffn(h1, wgu, wdn)
        by, sums, mine = dy[0], [None] * (2 * layers), None
        for layer in reversed(range(layers)):
            h, q, k, val, o, lse, h1, wa, wgu, wdn = kept[layer]
            if mine is None:
                by, do, delta, rest = ffn_back(by, h1, o, wgu, wdn, wa, n)
            else:
                by, do, delta, rest, sums[2 * layer + 2] = ffn_back(by, h1, o, wgu, wdn, wa, n, mine, next(ids))
            *onward, mine, sums[2 * layer + 1] = attend_back(q, k, val, do, lse, delta, h, c, s, wa, by if layer else None, rest, n, next(ids))
            by = onward[0] if onward else None
        sums[0], square = last(mine, sums[1:], n, next(ids))
        return tuple(adamw(sums, square, weights, m, v, n))

    states, cut = P(("rep", "dp"), None, None), P(None, "dp", None)
    return jax.shard_map(
        step,
        mesh=mesh,
        in_specs=(states, states) + (cut,) * 21,
        out_specs=(P("rep", "dp", None),) * 21,
        check_vma=False,
    )
```
